512 devices in a mesh: grid: 64 (over y, z), col: 8 (over x, core).
Axes of the slice: x: 4, y: 8, z: 8, core: 2. Of those that a mesh axis runs over, the one named last changes fastest.
Arguments:
- density: bfloat16 [196608, 1024], P('grid', 'col'), may hold values from -0.029907227 to 0.029907227
- row_centers: float32 [3, 196608], P(None, 'grid'), may hold values from -2 to 2
- row_exps: float32 [196608], P('grid'), may hold values from 0.2 to 1
- win_centers: float32 [3, 1024], P(None, 'col'), may hold values from -2 to 2
- win_exps: float32 [1024], P('col'), may hold values from 0.2 to 1
- points: float32 [256, 3, 128], P('grid'), may hold values from -2 to 2
- weights: float32 [256, 128], P('grid'), may hold values from 0.05 to 0.5
- sig_blocks: int32 [256, 32], replicated, may hold values from 0 to 1535, as said below
- pair_target: int32 [256, 16384], P('grid', 'col'), may hold values from 0 to 1023
- pair_source: int32 [256, 16384], P('grid', 'col'), may hold values from 0 to 127
Outputs:
- fock: float32 [196608, 1024], P('grid', 'col')
The draws below stay inside these ranges and needn't reach their ends.
Inputs may be any that keep to these rules, and one draw needn't show every extreme that they name: `sig_blocks`: each row lists 32 different blocks; block i is owned by grid index i // 24. Over the 4 rows of one grid index d (rows d * 4 to (d + 1) * 4 - 1, the batches that index holds), at most 2 different blocks of any one owner appear, and exactly 2 for some owner.
All inputs are finite; a program needn't handle non-finite values.
Results may differ from the reference program's by a relative error of at most 0.0011.
Values may be sent and summed in bfloat16 or wider, within the bound.
No kernel may reach another device: no remote copies, remote signals or barrier semaphores. Data moves between devices by JAX's collectives and lax.ppermute only.
A program may use at most 64 MiB of HBM per device.

```python
import math
import jax
import jax.numpy as jnp
from jax import lax

BLK = 128
PTS = 128
CAPB = 2
BLK_DEV = 24
S = 32
BPD = 4
COLW_DEV = 128
NBF = 196608
NCOLW = 1024
BATCHES = 256
NPAIR_ALL = 16384
N_GRID = 64
N_COL = 8


def draw_sig_blocks(key, part):
    owner_key, batch_key = jax.random.split(jax.random.fold_in(key, 11))
    owner_scores = jax.random.randint(owner_key, (N_GRID, N_GRID, BLK_DEV), 0, 2 ** 20) * BLK_DEV + jnp.arange(BLK_DEV, dtype=jnp.int32)
    chosen_local = jnp.argsort(owner_scores, axis=2)[:, :, :CAPB]
    pool = chosen_local + (jnp.arange(N_GRID, dtype=jnp.int32) * BLK_DEV)[None, :, None]
    pool_size = CAPB * N_GRID
    pool = pool.reshape(N_GRID, pool_size)
    positions = jnp.arange(pool_size, dtype=jnp.int32)
    pick_scores = jax.random.randint(batch_key, (N_GRID, BPD, pool_size), 0, 2 ** 20) * pool_size + positions[None, None, :]
    next_owner = (jnp.arange(N_GRID, dtype=jnp.int32) + 1) % N_GRID
    forced = positions[None, :] // CAPB == next_owner[:, None]
    first_batch = jnp.arange(BPD, dtype=jnp.int32) == 0
    forced_all = forced[:, None, :] & first_batch[None, :, None]
    pick_scores = jnp.where(forced_all, -1 - positions[None, None, :] % CAPB, pick_scores)
    order = jnp.argsort(pick_scores, axis=2)[:, :, :S]
    pool_wide = jnp.broadcast_to(pool[:, None, :], (N_GRID, BPD, pool_size))
    chosen = jnp.take_along_axis(pool_wide, order, axis=2)
    return chosen.reshape(N_GRID * BPD, S).astype(jnp.int32)


def plant(values, stream_key, least, high):
    longest = values.shape.index(max(values.shape))
    spots = []
    for shift in (0, 1):
        where = [jax.random.randint(jax.random.fold_in(stream_key, axis), (), 0, length) for axis, length in enumerate(values.shape)]
        where[longest] = (where[longest] + shift) % values.shape[longest]
        spots.append(tuple(where))
    return values.at[spots[0]].set(least).at[spots[1]].set(high)


def block_scale(key, dims, cuts, least, largest):
    factor_of, own = 1.0, jax.random.fold_in(key, 6)
    for axis_at, parts in cuts:
        draws = jnp.exp(jax.random.uniform(jax.random.fold_in(own, axis_at), (parts,), jnp.float32, least / len(cuts), largest / len(cuts)))
        factor_of = factor_of * jnp.repeat(draws, dims[axis_at] // parts).reshape([-1 if axis == axis_at else 1 for axis in range(len(dims))])
    return factor_of


def noise(key, dims, width, bound, shards=(), held_as=jnp.bfloat16):
    values = width * jax.random.normal(key, dims, jnp.float32)
    if shards:
        values = values * block_scale(key, dims, shards, -0.22, 0.18)
    return jnp.clip(values, -bound, bound).astype(held_as)


def setup_inputs(seed: int = 0) -> dict:
    splits = jax.random.split(jax.random.key(seed), 11)
    return {
        "density": noise(splits[0], (NBF, NCOLW), 0.005, 0.029907227, ((0, 64), (1, 8))),
        "row_centers": jnp.clip(jax.random.uniform(splits[1], (3, NBF), jnp.float32, -2.0, 2.0) * block_scale(splits[1], (3, NBF), ((1, 64),), -0.4, 0.0), -2.0, 2.0),
        "row_exps": jnp.clip(jnp.exp(math.log(1.0) - 1.609438 * jax.random.uniform(splits[2], (NBF,), jnp.float32) ** block_scale(splits[2], (NBF,), ((0, 64),), -0.2, 0.2)), 0.2, 1.0),
        "win_centers": jnp.clip(jax.random.uniform(splits[3], (3, NCOLW), jnp.float32, -2.0, 2.0) * block_scale(splits[3], (3, NCOLW), ((1, 8),), -0.4, 0.0), -2.0, 2.0),
        "win_exps": jnp.clip(jnp.exp(math.log(1.0) - 1.609438 * jax.random.uniform(splits[4], (NCOLW,), jnp.float32) ** block_scale(splits[4], (NCOLW,), ((0, 8),), -0.2, 0.2)), 0.2, 1.0),
        "points": jnp.clip(jax.random.uniform(splits[5], (BATCHES, 3, PTS), jnp.float32, -2.0, 2.0) * block_scale(splits[5], (BATCHES, 3, PTS), ((0, 64),), -0.4, 0.0), -2.0, 2.0),
        "weights": jnp.clip(jnp.exp(math.log(0.5) - 2.3025851 * jax.random.uniform(splits[6], (BATCHES, PTS), jnp.float32) ** block_scale(splits[6], (BATCHES, PTS), ((0, 64),), -0.2, 0.2)), 0.05, 0.5),
        "sig_blocks": draw_sig_blocks(jax.random.fold_in(splits[10], 71), 0),
        "pair_target": plant(jax.random.randint(splits[8], (BATCHES, NPAIR_ALL), 0, NCOLW), jax.random.fold_in(splits[8], 1), 0, NCOLW - 1).astype(jnp.int32),
        "pair_source": plant(jax.random.randint(splits[9], (BATCHES, NPAIR_ALL), 0, COLW_DEV), jax.random.fold_in(splits[9], 1), 0, COLW_DEV - 1).astype(jnp.int32),
    }


quad_nodes = 8


def boys_zero(argument):
    summed = jnp.zeros_like(argument)
    for quad_node in range(quad_nodes):
        node_spot = (quad_node + 0.5) / quad_nodes
        summed = summed + jnp.exp(-argument * (node_spot * node_spot))
    return summed / quad_nodes


def basis_values(centers, exponents, coordinates):
    squared = None
    for axis_id in range(3):
        deltas = coordinates[..., axis_id, :, None] - centers[..., axis_id, None, :]
        squared = deltas * deltas if squared is None else squared + deltas * deltas
    return jnp.exp(-exponents[..., None, :] * squared)


def pair_values(target_par, source_par, coordinates):
    target_exp = target_par[..., 3, :]
    source_exp = source_par[..., 3, :]
    joined = target_exp + source_exp
    separation = jnp.zeros_like(joined)
    spread = None
    for axis_id in range(3):
        offset = target_par[..., axis_id, :] - source_par[..., axis_id, :]
        separation = separation + offset * offset
        centre = (target_exp * target_par[..., axis_id, :] + source_exp * source_par[..., axis_id, :]) / joined
        deltas = coordinates[..., axis_id, :, None] - centre[..., None, :]
        spread = deltas * deltas if spread is None else spread + deltas * deltas
    prefactor = (2.0 * math.pi / joined) * jnp.exp(-target_exp * source_exp / joined * separation)
    return prefactor[..., None, :] * boys_zero(joined[..., None, :] * spread)


def reference(density, row_centers, row_exps, win_centers, win_exps, points, weights, sig_blocks, pair_target, pair_source):
    window = jnp.concatenate([win_centers, win_exps[None, :]], axis=0)
    row_params = jnp.concatenate([row_centers, row_exps[None, :]], axis=0)
    column_count = density.shape[1]
    local_width = column_count // N_COL
    per_column = pair_target.shape[1] // N_COL
    source_global = pair_source + (jnp.arange(pair_target.shape[1], dtype=jnp.int32) // per_column * local_width)[None, :]

    def one_batch(fock_sum, inputs):
        listing, coordinates, point_weights, target, source = inputs
        row_ids = (listing[:, None] * BLK + jnp.arange(BLK, dtype=jnp.int32)[None, :]).reshape(-1).astype(jnp.int32)
        row_tiles = jnp.take(density, row_ids, axis=0).astype(jnp.float32)
        params = jnp.take(row_params, row_ids, axis=1)
        basis_rows = basis_values(params[0:3], params[3], coordinates).astype(jnp.bfloat16)
        field_values = jnp.dot(basis_rows.astype(jnp.float32), row_tiles, preferred_element_type=jnp.float32, precision=lax.Precision.HIGHEST).astype(jnp.bfloat16)
        target_par = jnp.take(window, target, axis=1)
        source_par = jnp.take(window, source, axis=1)
        field_source = jnp.take(field_values, source, axis=1).astype(jnp.float32)
        product = (pair_values(target_par, source_par, coordinates) * field_source).astype(jnp.bfloat16)
        potential = jnp.zeros((coordinates.shape[1], column_count), jnp.float32).at[:, target].add(product.astype(jnp.float32))
        weighted = (point_weights[:, None] * potential).astype(jnp.bfloat16)
        contribution = jnp.dot(basis_rows.astype(jnp.float32).T, weighted.astype(jnp.float32), preferred_element_type=jnp.float32, precision=lax.Precision.HIGHEST)
        return fock_sum.at[row_ids].add(contribution), None

    zero_fock = jnp.zeros(density.shape, jnp.float32)
    fock_sum, unused = lax.scan(one_batch, zero_fock, (sig_blocks, points, weights, pair_target, source_global))
    return fock_sum
```

```python
import functools
import math

import jax
import jax.numpy as jnp
from jax import lax
from jax.experimental import pallas as pl
from jax.experimental.pallas import tpu as pltpu
from jax.sharding import PartitionSpec as P

BLK = 128
CAPB = 2
PARAMS = 4
CHUNK = 512
STEP_OWNERS = 4
SCALE_ROWS = 16
quad_nodes = 8
F32 = jnp.float32
BF16 = jnp.bfloat16


def call(kernel, name, flops=0, **kwargs):
    return pl.pallas_call(
        kernel,
        name=name,
        compiler_params=pltpu.CompilerParams(dimension_semantics=("arbitrary",) * len(kwargs["grid_spec"].grid)),
        cost_estimate=pl.CostEstimate(flops=flops, transcendentals=0, bytes_accessed=0),
        **kwargs,
    )


def pack_kernel(pick, tiles, params, tiles_out, params_out, *, owners_here):
    base = pl.program_id(0) * owners_here
    for owner in range(owners_here):
        for slot in range(CAPB):
            block = pick[(base + owner) * CAPB + slot]
            tiles_out[owner, slot * BLK : (slot + 1) * BLK, :] = tiles[block]
            params_out[owner, slot * PARAMS : (slot + 1) * PARAMS, :] = params[block]


def pack_slots(pick, tiles, params, owners):
    held, _, width = tiles.shape
    owners_here = min(8, owners)
    return call(
        functools.partial(pack_kernel, owners_here=owners_here),
        "pack_slots",
        grid_spec=pltpu.PrefetchScalarGridSpec(
            num_scalar_prefetch=1,
            grid=(owners // owners_here,),
            in_specs=[
                pl.BlockSpec((held, BLK, width), lambda i, *_: (0, 0, 0)),
                pl.BlockSpec((held, PARAMS, BLK), lambda i, *_: (0, 0, 0)),
            ],
            out_specs=[
                pl.BlockSpec((owners_here, CAPB * BLK, width), lambda i, *_: (i, 0, 0)),
                pl.BlockSpec((owners_here, CAPB * PARAMS, BLK), lambda i, *_: (i, 0, 0)),
            ],
        ),
        out_shape=[
            jax.ShapeDtypeStruct((owners, CAPB * BLK, width), BF16),
            jax.ShapeDtypeStruct((owners, CAPB * PARAMS, BLK), F32),
        ],
    )(pick, tiles, params)


def basis_kernel(slots, params, points, out, spots, *, listed):
    batch = pl.program_id(0)
    for axis in range(3):
        spots[axis] = jnp.broadcast_to(points[0, :, axis : axis + 1], spots.shape[1:])

    def one_block(entry, carry):
        row = slots[batch * listed + entry] * PARAMS
        squared = None
        for axis in range(3):
            delta = spots[axis] - params[pl.ds(row + axis, 1), :]
            squared = delta * delta if squared is None else squared + delta * delta
        value = jnp.exp(-params[pl.ds(row + 3, 1), :] * squared)
        out[0, :, pl.ds(pl.multiple_of(entry * BLK, BLK), BLK)] = value.astype(BF16)
        return carry

    lax.fori_loop(0, listed, one_block, 0, unroll=2)


def basis_for_field(slots, params, points_t, listed):
    batches, pts, _ = points_t.shape
    return call(
        functools.partial(basis_kernel, listed=listed),
        "basis_for_field",
        flops=batches * pts * listed * BLK * 100,
        grid_spec=pltpu.PrefetchScalarGridSpec(
            num_scalar_prefetch=1,
            grid=(batches,),
            in_specs=[
                pl.BlockSpec(params.shape, lambda b, *_: (0, 0)),
                pl.BlockSpec((1, pts, 3), lambda b, *_: (b, 0, 0)),
            ],
            out_specs=pl.BlockSpec((1, pts, listed * BLK), lambda b, *_: (b, 0, 0)),
            scratch_shapes=[pltpu.VMEM((3, pts, BLK), F32)],
        ),
        out_shape=jax.ShapeDtypeStruct((batches, pts, listed * BLK), BF16),
    )(slots, params, points_t)


def one_hot(columns, rows):
    spot = lax.broadcasted_iota(jnp.int32, (rows, columns.shape[1]), 0)
    return jnp.where(spot == columns, 1.0, 0.0).astype(BF16)


def rejoin(picked):
    return picked[0:4] + picked[4:8] + picked[8:12]


def pair_kernel(target, source, window, local, points, out, spots):
    @pl.when(pl.program_id(1) == 0)
    def _():
        for axis in range(3):
            spots[axis] = jnp.broadcast_to(points[0, :, axis : axis + 1], spots.shape[1:])

    target_par = rejoin(
        jnp.dot(window[...], one_hot(target[0], window.shape[1]), preferred_element_type=F32)
    )
    source_par = rejoin(
        jnp.dot(local[...], one_hot(source[0], local.shape[1]), preferred_element_type=F32)
    )
    target_exp, source_exp = target_par[3:4], source_par[3:4]
    joined = target_exp + source_exp
    separation = jnp.zeros_like(joined)
    centres = []
    for axis in range(3):
        here, there = target_par[axis : axis + 1], source_par[axis : axis + 1]
        offset = here - there
        separation = separation + offset * offset
        centres.append((target_exp * here + source_exp * there) / joined)
    prefactor = 2.0 * math.pi / joined * jnp.exp(-target_exp * source_exp / joined * separation)
    lanes = spots.shape[2]
    for first in range(0, joined.shape[1], lanes):
        part = slice(first, first + lanes)
        spread = None
        for axis in range(3):
            delta = spots[axis] - centres[axis][:, part]
            spread = delta * delta if spread is None else spread + delta * delta
        argument = joined[:, part] * spread
        summed = jnp.zeros_like(argument)
        for quad_node in range(quad_nodes):
            node_spot = (quad_node + 0.5) / quad_nodes
            summed = summed + jnp.exp(-argument * (node_spot * node_spot))
        out[0, :, part] = prefactor[:, part] * (summed / quad_nodes)


def pair_values(target, source, window, local, points_t):
    batches, _, pairs = target.shape
    pts = points_t.shape[1]
    return call(
        pair_kernel,
        "pair_values",
        flops=batches * pairs * pts * 400,
        grid_spec=pltpu.PrefetchScalarGridSpec(
            num_scalar_prefetch=0,
            grid=(batches, pairs // CHUNK),
            in_specs=[
                pl.BlockSpec((1, 1, CHUNK), lambda b, n: (b, 0, n)),
                pl.BlockSpec((1, 1, CHUNK), lambda b, n: (b, 0, n)),
                pl.BlockSpec(window.shape, lambda b, n: (0, 0)),
                pl.BlockSpec(local.shape, lambda b, n: (0, 0)),
                pl.BlockSpec((1, pts, 3), lambda b, n: (b, 0, 0)),
            ],
            out_specs=pl.BlockSpec((1, pts, CHUNK), lambda b, n: (b, 0, n)),
            scratch_shapes=[pltpu.VMEM((3, pts, BLK), F32)],
        ),
        out_shape=jax.ShapeDtypeStruct((batches, pts, pairs), F32),
    )(target, source, window, local, points_t)


def potential_kernel(slots, tiles, basis, values, target, source, out, rows, *, listed):
    batch = pl.program_id(0)
    for entry in range(listed):
        first = pl.multiple_of(slots[batch * listed + entry] * BLK, BLK)
        rows[entry * BLK : (entry + 1) * BLK, :] = tiles[pl.ds(first, BLK), :]
    field = jnp.dot(basis[0], rows[...], preferred_element_type=F32).astype(BF16)
    columns, width = out.shape[0], out.shape[3]
    window_count = columns * width
    potential = jnp.zeros((field.shape[0], window_count), F32)
    for first in range(0, values.shape[2], CHUNK):
        part = slice(first, first + CHUNK)
        picked = jnp.dot(field, one_hot(source[0, :, part], width), preferred_element_type=F32)
        product = (values[0, :, part] * picked).astype(BF16)
        potential += lax.dot_general(
            product,
            one_hot(target[0, :, part], window_count),
            (((1,), (1,)), ((), ())),
            preferred_element_type=F32,
        )
    for column in range(columns):
        out[column, 0] = potential[:, column * width : (column + 1) * width]


def potential_parts(slots, tiles, basis, values, target, source, columns):
    batches, pts, functions = basis.shape
    pairs = values.shape[2]
    width = tiles.shape[1]
    return call(
        functools.partial(potential_kernel, listed=functions // BLK),
        "potential_parts",
        grid_spec=pltpu.PrefetchScalarGridSpec(
            num_scalar_prefetch=1,
            grid=(batches,),
            in_specs=[
                pl.BlockSpec(tiles.shape, lambda b, *_: (0, 0)),
                pl.BlockSpec((1, pts, functions), lambda b, *_: (b, 0, 0)),
                pl.BlockSpec((1, pts, pairs), lambda b, *_: (b, 0, 0)),
                pl.BlockSpec((1, 1, pairs), lambda b, *_: (b, 0, 0)),
                pl.BlockSpec((1, 1, pairs), lambda b, *_: (b, 0, 0)),
            ],
            out_specs=pl.BlockSpec((columns, 1, pts, width), lambda b, *_: (0, b, 0, 0)),
            scratch_shapes=[pltpu.VMEM((functions, width), BF16)],
        ),
        out_shape=jax.ShapeDtypeStruct((columns, batches, pts, width), F32),
    )(slots, tiles, basis, values, target, source)


def owner_basis_kernel(pick, listed, params, points, out, spread_params, *, batches):
    @pl.when(pl.program_id(0) == 0)
    def _():
        for block in range(spread_params.shape[0]):
            for which in range(PARAMS):
                spread_params[block, which] = jnp.broadcast_to(
                    params[block * BLK : (block + 1) * BLK, which : which + 1], (BLK, BLK)
                )

    def one_owner(owner, carry):
        place = pl.program_id(0) * STEP_OWNERS + owner
        for slot in range(CAPB):
            block = pick[place * CAPB + slot]
            for batch in range(batches):
                squared = None
                for axis in range(3):
                    row = axis * batches + batch
                    delta = points[owner, row : row + 1, :] - spread_params[block, axis]
                    squared = delta * delta if squared is None else squared + delta * delta
                value = jnp.exp(-spread_params[block, 3] * squared)
                keep = listed[(place * CAPB + slot) * batches + batch]
                value = jnp.where(keep > 0, value, 0.0)
                out[owner, slot * BLK : (slot + 1) * BLK, batch * BLK : (batch + 1) * BLK] = (
                    value.astype(BF16)
                )
        return carry

    lax.fori_loop(0, STEP_OWNERS, one_owner, 0)


def basis_at_owner(pick, listed, params_t, points_all, batches):
    owners, rows, pts = points_all.shape
    held = params_t.shape[0] // BLK
    return call(
        functools.partial(owner_basis_kernel, batches=batches),
        "basis_at_owner",
        flops=owners * CAPB * BLK * batches * pts * 100,
        grid_spec=pltpu.PrefetchScalarGridSpec(
            num_scalar_prefetch=2,
            grid=(owners // STEP_OWNERS,),
            in_specs=[
                pl.BlockSpec(params_t.shape, lambda i, *_: (0, 0)),
                pl.BlockSpec((STEP_OWNERS, rows, pts), lambda i, *_: (i, 0, 0)),
            ],
            out_specs=pl.BlockSpec((STEP_OWNERS, CAPB * BLK, batches * pts), lambda i, *_: (i, 0, 0)),
            scratch_shapes=[pltpu.VMEM((held, PARAMS, BLK, BLK), F32)],
        ),
        out_shape=jax.ShapeDtypeStruct((owners, CAPB * BLK, batches * pts), BF16),
    )(pick, listed, params_t, points_all)


def fock_kernel(pick, basis, weighted, out):
    @pl.when(pl.program_id(0) == 0)
    def _():
        out[...] = jnp.zeros_like(out)

    for owner in range(STEP_OWNERS):
        place = pl.program_id(0) * STEP_OWNERS + owner
        rows = jnp.dot(basis[owner], weighted[owner], preferred_element_type=F32)
        for slot in range(CAPB):
            block = pick[place * CAPB + slot]
            out[block] = out[block] + rows[slot * BLK : (slot + 1) * BLK]


def fock_at_owner(pick, basis, weighted, held):
    owners, rows, points = basis.shape
    width = weighted.shape[2]
    return call(
        fock_kernel,
        "fock_at_owner",
        flops=2 * owners * rows * points * width,
        grid_spec=pltpu.PrefetchScalarGridSpec(
            num_scalar_prefetch=1,
            grid=(owners // STEP_OWNERS,),
            in_specs=[
                pl.BlockSpec((STEP_OWNERS, rows, points), lambda i, *_: (i, 0, 0)),
                pl.BlockSpec((STEP_OWNERS, points, width), lambda i, *_: (i, 0, 0)),
            ],
            out_specs=pl.BlockSpec((held, BLK, width), lambda i, *_: (0, 0, 0)),
        ),
        out_shape=jax.ShapeDtypeStruct((held, BLK, width), F32),
    )(pick, basis, weighted)


def to_everyone(value, axis):
    devices = lax.axis_size(axis)
    return lax.all_to_all(
        jnp.broadcast_to(value[None], (devices, *value.shape)), axis, 0, 0, tiled=True
    )


def in_parts(values):
    high = lax.reduce_precision(values, 8, 7)
    middle = lax.reduce_precision(values - high, 8, 7)
    low = values - high - middle
    parts = jnp.concatenate([high, middle, low, jnp.zeros_like(low)], axis=0)
    return parts.astype(BF16)


def sum_at_column(parts):
    columns, batches, pts, width = parts.shape
    largest = jnp.max(jnp.abs(parts), axis=(0, 2, 3))
    power = jnp.clip(13.0 - jnp.ceil(jnp.log2(largest)), -100.0, 100.0)
    scaled = (parts * jnp.exp2(power)[None, :, None, None]).astype(jnp.float16)
    tail = jnp.broadcast_to(
        power[None, :, None, None], (columns, batches, SCALE_ROWS, width)
    ).astype(jnp.float16)
    got = lax.all_to_all(
        jnp.concatenate([scaled, tail], axis=2), "col", split_axis=0, concat_axis=0, tiled=True
    )
    factor = jnp.exp2(-got[:, :, pts : pts + 1, 0:1].astype(F32))
    return jnp.sum(got[:, :, :pts].astype(F32) * factor, axis=0)


def on_device(
    density,
    row_centers,
    row_exps,
    win_centers,
    win_exps,
    points,
    weights,
    sig_blocks,
    pair_target,
    pair_source,
):
    owners = lax.axis_size("grid")
    columns = lax.axis_size("col")
    my_index = lax.axis_index("grid")
    held = row_exps.shape[0] // BLK
    width = density.shape[1]
    batches, _, pts = points.shape
    listed = sig_blocks.shape[1]

    lists = sig_blocks.reshape(owners, batches * listed)
    spot = lists - my_index * held
    owned = (spot >= 0) & (spot < held)
    lowest = jnp.min(jnp.where(owned, spot, held), axis=1)
    highest = jnp.max(jnp.where(owned, spot, -1), axis=1)
    found = highest >= 0
    ends = jnp.stack([lowest, highest], axis=1)
    pick = jnp.where(found[:, None], ends, 0).reshape(-1).astype(jnp.int32)
    at_end = owned[:, None, :] & (spot[:, None, :] == ends[:, :, None])
    at_end = at_end & ((ends[:, 1:] != ends[:, :1]) | (jnp.arange(CAPB) == 0))[:, :, None]
    in_batch = jnp.any(at_end.reshape(owners, CAPB, batches, listed), axis=3)
    in_batch = in_batch.reshape(-1).astype(jnp.int32)

    mine = lax.dynamic_slice_in_dim(lists, my_index, 1, 0)[0]
    owner_of = mine // held
    second = jnp.any(
        (owner_of[:, None] == owner_of[None, :]) & (mine[None, :] < mine[:, None]), axis=1
    )
    slots = (owner_of * CAPB + second).astype(jnp.int32)

    own_params = jnp.concatenate([row_centers, row_exps[None, :]], axis=0)
    own_blocks = own_params.reshape(PARAMS, held, BLK).transpose(1, 0, 2)
    tile_slots, param_slots = pack_slots(
        pick, density.reshape(held, BLK, width), own_blocks, owners
    )
    got_params = lax.all_to_all(param_slots, "grid", split_axis=0, concat_axis=0, tiled=True)
    got_tiles = lax.all_to_all(tile_slots, "grid", split_axis=0, concat_axis=0, tiled=True)

    points_t = points.transpose(0, 2, 1)
    basis = basis_for_field(
        slots, got_params.reshape(owners * CAPB * PARAMS, BLK), points_t, listed
    )
    local_window = jnp.concatenate([win_centers, win_exps[None, :]], axis=0)
    whole_window = to_everyone(local_window, "col").transpose(1, 0, 2).reshape(PARAMS, -1)
    target = pair_target[:, None, :]
    source = pair_source[:, None, :]
    values = pair_values(target, source, in_parts(whole_window), in_parts(local_window), points_t)
    parts = potential_parts(
        slots,
        got_tiles.reshape(owners * CAPB * BLK, width),
        basis,
        values,
        target,
        source,
        columns,
    )
    potential = sum_at_column(parts)
    weighted = (weights[:, :, None] * potential).astype(BF16).reshape(batches * pts, width)

    all_weighted = lax.all_gather(weighted, "grid", axis=0, tiled=True)
    points_all = to_everyone(points.transpose(1, 0, 2).reshape(3 * batches, pts), "grid")
    own_basis = basis_at_owner(pick, in_batch, own_params.T, points_all, batches)
    fock = fock_at_owner(
        pick, own_basis, all_weighted.reshape(owners, batches * pts, width), held
    )
    return fock.reshape(held * BLK, width)


def solution(mesh):
    return jax.shard_map(
        on_device,
        mesh=mesh,
        in_specs=(
            P("grid", "col"),
            P(None, "grid"),
            P("grid"),
            P(None, "col"),
            P("col"),
            P("grid", None, None),
            P("grid", None),
            P(),
            P("grid", "col"),
            P("grid", "col"),
        ),
        out_specs=P("grid", "col"),
        check_vma=False,
    )
```

```python
import functools
import math

import jax
import jax.numpy as jnp
from jax import lax
from jax.experimental import pallas as pl
from jax.experimental.pallas import tpu as pltpu
from jax.sharding import Mesh
from jax.sharding import PartitionSpec as P

BLK = 128
CAPB = 2
PARAMS = 4
CHUNK = 512
STEP_OWNERS = 4
SCALE_ROWS = 16
POINT_ROWS = 16
GRID = ("y", "z")
quad_nodes = 8
F32 = jnp.float32
BF16 = jnp.bfloat16


def call(kernel, name, flops=0, **kwargs):
    return pl.pallas_call(
        kernel,
        name=name,
        compiler_params=pltpu.CompilerParams(
            dimension_semantics=("arbitrary",) * len(kwargs["grid_spec"].grid),
        ),
        cost_estimate=pl.CostEstimate(flops=flops, transcendentals=0, bytes_accessed=0),
        **kwargs,
    )


def pack_kernel(pick, tiles, out):
    first = pl.program_id(0) * out.shape[0]
    for owner in range(out.shape[0]):
        for slot in range(CAPB):
            out[owner, slot * BLK : (slot + 1) * BLK, :] = tiles[pick[(first + owner) * CAPB + slot]]


def pack_slots(pick, tiles, owners):
    held, _, width = tiles.shape
    owners_here = min(8, owners)
    return call(
        pack_kernel,
        "pack_slots",
        grid_spec=pltpu.PrefetchScalarGridSpec(
            num_scalar_prefetch=1,
            grid=(owners // owners_here,),
            in_specs=[pl.BlockSpec((held, BLK, width), lambda i, *_: (0, 0, 0))],
            out_specs=pl.BlockSpec((owners_here, CAPB * BLK, width), lambda i, *_: (i, 0, 0)),
        ),
        out_shape=jax.ShapeDtypeStruct((owners, CAPB * BLK, width), BF16),
    )(pick, tiles)


def basis_kernel(rows_at, params, points, out, spots, *, listed):
    batch = pl.program_id(0)
    for axis in range(3):
        spots[axis] = jnp.broadcast_to(points[0, :, axis : axis + 1], spots.shape[1:])

    def one_block(entry, carry):
        row = rows_at[batch * listed + entry]
        squared = None
        for axis in range(3):
            delta = spots[axis] - params[pl.ds(row + axis, 1), :]
            squared = delta * delta if squared is None else squared + delta * delta
        value = jnp.exp(-params[pl.ds(row + 3, 1), :] * squared)
        out[0, :, pl.ds(pl.multiple_of(entry * BLK, BLK), BLK)] = value.astype(BF16)
        return carry

    lax.fori_loop(0, listed, one_block, 0, unroll=2)


def basis_for_field(rows_at, params, points_t, listed):
    batches, pts, _ = points_t.shape
    return call(
        functools.partial(basis_kernel, listed=listed),
        "basis_for_field",
        flops=batches * pts * listed * BLK * 100,
        grid_spec=pltpu.PrefetchScalarGridSpec(
            num_scalar_prefetch=1,
            grid=(batches,),
            in_specs=[
                pl.BlockSpec(params.shape, lambda b, *_: (0, 0)),
                pl.BlockSpec((1, pts, 3), lambda b, *_: (b, 0, 0)),
            ],
            out_specs=pl.BlockSpec((1, pts, listed * BLK), lambda b, *_: (b, 0, 0)),
            scratch_shapes=[pltpu.VMEM((3, pts, BLK), F32)],
        ),
        out_shape=pltpu.HBM((batches, pts, listed * BLK), BF16),
    )(rows_at, params, points_t)


def one_hot(columns, rows):
    spot = lax.broadcasted_iota(jnp.int32, (rows, columns.shape[1]), 0)
    return jnp.where(spot == columns, 1.0, 0.0).astype(BF16)


def rejoin(picked):
    return picked[0:4] + picked[4:8] + picked[8:12]


def pair_kernel(target, source, window, local, points, out, spots):
    @pl.when(pl.program_id(1) == 0)
    def _():
        for axis in range(3):
            spots[axis] = jnp.broadcast_to(points[0, :, axis : axis + 1], spots.shape[1:])

    target_par = rejoin(
        jnp.dot(window[...], one_hot(target[0], window.shape[1]), preferred_element_type=F32)
    )
    source_par = rejoin(
        jnp.dot(local[...], one_hot(source[0], local.shape[1]), preferred_element_type=F32)
    )
    target_exp, source_exp = target_par[3:4], source_par[3:4]
    joined = target_exp + source_exp
    separation = jnp.zeros_like(joined)
    centres = []
    for axis in range(3):
        here, there = target_par[axis : axis + 1], source_par[axis : axis + 1]
        offset = here - there
        separation = separation + offset * offset
        centres.append((target_exp * here + source_exp * there) / joined)
    prefactor = 2.0 * math.pi / joined * jnp.exp(-target_exp * source_exp / joined * separation)
    lanes = spots.shape[2]
    for first in range(0, joined.shape[1], lanes):
        part = slice(first, first + lanes)
        spread = None
        for axis in range(3):
            delta = spots[axis] - centres[axis][:, part]
            spread = delta * delta if spread is None else spread + delta * delta
        argument = joined[:, part] * spread
        summed = jnp.zeros_like(argument)
        for quad_node in range(quad_nodes):
            node_spot = (quad_node + 0.5) / quad_nodes
            summed = summed + jnp.exp(-argument * (node_spot * node_spot))
        out[0, :, part] = prefactor[:, part] * (summed / quad_nodes)


def pair_values(target, source, window, local, points_t):
    batches, _, pairs = target.shape
    pts = points_t.shape[1]
    return call(
        pair_kernel,
        "pair_values",
        flops=batches * pairs * pts * 400,
        grid_spec=pltpu.PrefetchScalarGridSpec(
            num_scalar_prefetch=0,
            grid=(batches, pairs // CHUNK),
            in_specs=[
                pl.BlockSpec((1, 1, CHUNK), lambda b, n: (b, 0, n)),
                pl.BlockSpec((1, 1, CHUNK), lambda b, n: (b, 0, n)),
                pl.BlockSpec(window.shape, lambda b, n: (0, 0)),
                pl.BlockSpec(local.shape, lambda b, n: (0, 0)),
                pl.BlockSpec((1, pts, 3), lambda b, n: (b, 0, 0)),
            ],
            out_specs=pl.BlockSpec((1, pts, CHUNK), lambda b, n: (b, 0, n)),
            scratch_shapes=[pltpu.VMEM((3, pts, BLK), F32)],
        ),
        out_shape=pltpu.HBM((batches, pts, pairs), F32),
    )(target, source, window, local, points_t)


def potential_kernel(slots, tiles, basis, values, target, source, out, rows, *, listed):
    batch = pl.program_id(0)
    for entry in range(listed):
        first = pl.multiple_of(slots[batch * listed + entry] * BLK, BLK)
        rows[entry * BLK : (entry + 1) * BLK, :] = tiles[pl.ds(first, BLK), :]
    field = jnp.dot(basis[0], rows[...], preferred_element_type=F32).astype(BF16)
    columns, width = out.shape[0], out.shape[3]
    window_count = columns * width
    potential = jnp.zeros((field.shape[0], window_count), F32)
    for first in range(0, values.shape[2], CHUNK):
        part = slice(first, first + CHUNK)
        picked = jnp.dot(field, one_hot(source[0, :, part], width), preferred_element_type=F32)
        product = (values[0, :, part] * picked).astype(BF16)
        potential += lax.dot_general(
            product,
            one_hot(target[0, :, part], window_count),
            (((1,), (1,)), ((), ())),
            preferred_element_type=F32,
        )
    for column in range(columns):
        out[column, 0] = potential[:, column * width : (column + 1) * width]


def potential_parts(slots, tiles, basis, values, target, source, columns):
    batches, pts, functions = basis.shape
    pairs = values.shape[2]
    width = tiles.shape[1]
    return call(
        functools.partial(potential_kernel, listed=functions // BLK),
        "potential_parts",
        grid_spec=pltpu.PrefetchScalarGridSpec(
            num_scalar_prefetch=1,
            grid=(batches,),
            in_specs=[
                pl.BlockSpec(tiles.shape, lambda b, *_: (0, 0)),
                pl.BlockSpec((1, pts, functions), lambda b, *_: (b, 0, 0)),
                pl.BlockSpec((1, pts, pairs), lambda b, *_: (b, 0, 0)),
                pl.BlockSpec((1, 1, pairs), lambda b, *_: (b, 0, 0)),
                pl.BlockSpec((1, 1, pairs), lambda b, *_: (b, 0, 0)),
            ],
            out_specs=pl.BlockSpec((columns, 1, pts, width), lambda b, *_: (0, b, 0, 0)),
            scratch_shapes=[pltpu.VMEM((functions, width), BF16)],
        ),
        out_shape=jax.ShapeDtypeStruct((columns, batches, pts, width), F32),
    )(slots, tiles, basis, values, target, source)


def owner_basis_kernel(pick, listed, params, points, out, spread_params, *, batches):
    @pl.when(pl.program_id(0) == 0)
    def _():
        for block in range(spread_params.shape[0]):
            for which in range(PARAMS):
                spread_params[block, which] = jnp.broadcast_to(
                    params[block * BLK : (block + 1) * BLK, which : which + 1], (BLK, BLK)
                )

    def one_owner(owner, carry):
        place = pl.program_id(0) * STEP_OWNERS + owner
        for slot in range(CAPB):
            block = pick[place * CAPB + slot]
            for batch in range(batches):
                here = (owner, slice(slot * BLK, (slot + 1) * BLK), slice(batch * BLK, (batch + 1) * BLK))
                keep = listed[(place * CAPB + slot) * batches + batch]

                @pl.when(keep > 0)
                def _():
                    squared = None
                    for axis in range(3):
                        row = axis * batches + batch
                        delta = points[owner, row : row + 1, :] - spread_params[block, axis]
                        squared = delta * delta if squared is None else squared + delta * delta
                    out[here] = jnp.exp(-spread_params[block, 3] * squared).astype(BF16)

                @pl.when(keep == 0)
                def _():
                    out[here] = jnp.zeros((BLK, BLK), BF16)

        return carry

    lax.fori_loop(0, STEP_OWNERS, one_owner, 0)


def basis_at_owner(pick, listed, params_t, gathered, batches, pts):
    owners, rows, _ = gathered.shape
    held = params_t.shape[0] // BLK
    return call(
        functools.partial(owner_basis_kernel, batches=batches),
        "basis_at_owner",
        flops=owners * CAPB * BLK * batches * pts * 100,
        grid_spec=pltpu.PrefetchScalarGridSpec(
            num_scalar_prefetch=2,
            grid=(owners // STEP_OWNERS,),
            in_specs=[
                pl.BlockSpec(params_t.shape, lambda i, *_: (0, 0)),
                pl.BlockSpec(
                    (STEP_OWNERS, POINT_ROWS, BLK), lambda i, *_: (i, rows // POINT_ROWS - 1, 0)
                ),
            ],
            out_specs=pl.BlockSpec((STEP_OWNERS, CAPB * BLK, batches * pts), lambda i, *_: (i, 0, 0)),
            scratch_shapes=[pltpu.VMEM((held, PARAMS, BLK, BLK), F32)],
        ),
        out_shape=pltpu.HBM((owners, CAPB * BLK, batches * pts), BF16),
    )(pick, listed, params_t, gathered)


def add_rows(out, pick, place, rows):
    for slot in range(CAPB):
        block = pick[place * CAPB + slot]
        out[block] = out[block] + rows[slot * BLK : (slot + 1) * BLK]


def fock_kernel(pick, basis, weighted, before, out):
    @pl.when(pl.program_id(0) == 0)
    def _():
        out[...] = before[...]

    for owner in range(STEP_OWNERS):
        place = pl.program_id(0) * STEP_OWNERS + owner
        add_rows(out, pick, place, jnp.dot(basis[owner], weighted[owner], preferred_element_type=F32))


def fock_from_gather(pick, basis, weighted, before):
    owners, rows, _ = basis.shape
    _, points, width = weighted.shape
    return call(
        fock_kernel,
        "fock_from_gather",
        flops=2 * owners * rows * points * width,
        grid_spec=pltpu.PrefetchScalarGridSpec(
            num_scalar_prefetch=1,
            grid=(owners // STEP_OWNERS,),
            in_specs=[
                pl.BlockSpec((STEP_OWNERS, rows, points), lambda i, *_: (i, 0, 0)),
                pl.BlockSpec((STEP_OWNERS, points, width), lambda i, *_: (i, 0, 0)),
                pl.BlockSpec(before.shape, lambda i, *_: (0, 0, 0)),
            ],
            out_specs=pl.BlockSpec(before.shape, lambda i, *_: (0, 0, 0)),
        ),
        out_shape=jax.ShapeDtypeStruct(before.shape, F32),
        input_output_aliases={3: 0},
    )(pick, basis, weighted, before)


def fock_line_kernel(pick, lines, *refs, first, count, side, fresh):
    basis, weighted, out = refs[:count], refs[count : 2 * count], refs[-1]

    @pl.when(pl.program_id(0) == 0)
    def _():
        out[...] = jnp.zeros_like(out) if fresh else refs[2 * count][...]

    for line in range(count):
        place = pl.program_id(0) * side + lines[first + line]
        rows = jnp.dot(basis[line][0, 0], weighted[line][0], preferred_element_type=F32)
        add_rows(out, pick, place, rows)


def fock_from_lines(pick, lines, first, basis, weighted, before, held):
    side, _, rows, _ = basis.shape
    count = len(weighted)
    _, points, width = weighted[0].shape
    last = basis.shape[3] // points - 1
    whole = pl.BlockSpec((held, BLK, width), lambda i, *_: (0, 0, 0))

    def line_spec(line):
        return pl.BlockSpec((1, 1, rows, points), lambda i, _, lines: (i, lines[first + line], 0, last))

    return call(
        functools.partial(
            fock_line_kernel, first=first, count=count, side=side, fresh=before is None
        ),
        "fock_from_lines",
        flops=2 * count * side * rows * points * width,
        grid_spec=pltpu.PrefetchScalarGridSpec(
            num_scalar_prefetch=2,
            grid=(side,),
            in_specs=[line_spec(line) for line in range(count)]
            + [pl.BlockSpec((1, points, width), lambda i, *_: (i, 0, 0))] * count
            + ([] if before is None else [whole]),
            out_specs=whole,
        ),
        out_shape=jax.ShapeDtypeStruct((held, BLK, width), F32),
        input_output_aliases={} if before is None else {2 + 2 * count: 0},
    )(pick, lines, *[basis] * count, *weighted, *([] if before is None else [before]))


def to_everyone(value, axis):
    devices = lax.axis_size(axis)
    return lax.all_to_all(
        jnp.broadcast_to(value[None], (devices, *value.shape)), axis, 0, 0, tiled=True
    )


def in_parts(values):
    high = lax.reduce_precision(values, 8, 7)
    middle = lax.reduce_precision(values - high, 8, 7)
    low = values - high - middle
    parts = jnp.concatenate([high, middle, low, jnp.zeros_like(low)], axis=0)
    return parts.astype(BF16)


def sum_at_column(parts):
    columns, batches, pts, width = parts.shape
    largest = jnp.max(jnp.abs(parts), axis=(0, 2, 3))
    power = jnp.clip(13.0 - jnp.ceil(jnp.log2(largest)), -100.0, 100.0)
    scaled = (parts * jnp.exp2(power)[None, :, None, None]).astype(jnp.float16)
    tail = jnp.broadcast_to(
        power[None, :, None, None], (columns, batches, SCALE_ROWS, width)
    ).astype(jnp.float16)
    got = lax.all_to_all(
        jnp.concatenate([scaled, tail], axis=2), "col", split_axis=0, concat_axis=0, tiled=True
    )
    factor = jnp.exp2(-got[:, :, pts : pts + 1, 0:1].astype(F32))
    return jnp.sum(got[:, :, :pts].astype(F32) * factor, axis=0)


def on_device(
    density,
    row_centers,
    row_exps,
    win_centers,
    win_exps,
    points,
    weights,
    sig_blocks,
    pair_target,
    pair_source,
):
    owners = lax.axis_size(GRID)
    columns = lax.axis_size("col")
    my_index = lax.axis_index(GRID)
    held = row_exps.shape[0] // BLK
    width = density.shape[1]
    batches, _, pts = points.shape
    listed = sig_blocks.shape[1]

    lists = sig_blocks.reshape(owners, batches * listed)
    spot = lists - my_index * held
    owned = (spot >= 0) & (spot < held)
    lowest = jnp.min(jnp.where(owned, spot, held), axis=1)
    highest = jnp.max(jnp.where(owned, spot, -1), axis=1)
    found = highest >= 0
    ends = jnp.stack([lowest, highest], axis=1)
    pick = jnp.where(found[:, None], ends, 0).reshape(-1).astype(jnp.int32)
    at_end = owned[:, None, :] & (spot[:, None, :] == ends[:, :, None])
    at_end = at_end & ((ends[:, 1:] != ends[:, :1]) | (jnp.arange(CAPB) == 0))[:, :, None]
    in_batch = jnp.any(at_end.reshape(owners, CAPB, batches, listed), axis=3)
    in_batch = in_batch.reshape(-1).astype(jnp.int32)

    mine = lax.dynamic_slice_in_dim(lists, my_index, 1, 0)[0]
    owner_of = mine // held
    second = jnp.any(
        (owner_of[:, None] == owner_of[None, :]) & (mine[None, :] < mine[:, None]), axis=1
    )
    slots = (owner_of * CAPB + second).astype(jnp.int32)

    own_params = jnp.concatenate([row_centers, row_exps[None, :]], axis=0)
    own_blocks = own_params.reshape(PARAMS, held, BLK).transpose(1, 0, 2).reshape(-1, BLK)
    own_points = points.transpose(1, 0, 2).reshape(3 * batches, pts)
    spare = jnp.zeros((POINT_ROWS - own_points.shape[0], BLK), F32)
    sent = jnp.concatenate([own_blocks, own_points, spare], axis=0)
    gathered = lax.all_gather(sent, GRID, axis=0, tiled=True)
    rows_each = sent.shape[0]
    rows_at = (owner_of * rows_each + (mine - owner_of * held) * PARAMS).astype(jnp.int32)

    tile_slots = pack_slots(pick, density.reshape(held, BLK, width), owners)
    got_tiles = lax.all_to_all(tile_slots, GRID, split_axis=0, concat_axis=0, tiled=True)

    points_t = points.transpose(0, 2, 1)
    local_window = jnp.concatenate([win_centers, win_exps[None, :]], axis=0)
    whole_window = to_everyone(local_window, "col").transpose(1, 0, 2).reshape(PARAMS, -1)
    target = pair_target[:, None, :]
    source = pair_source[:, None, :]
    values = pair_values(target, source, in_parts(whole_window), in_parts(local_window), points_t)
    basis = basis_for_field(rows_at, gathered, points_t, listed)
    own_basis = basis_at_owner(
        pick, in_batch, own_params.T, gathered.reshape(owners, rows_each, BLK), batches, pts
    )
    basis, values, own_basis = lax.optimization_barrier((basis, values, own_basis))
    parts = potential_parts(
        slots,
        got_tiles.reshape(owners * CAPB * BLK, width),
        basis,
        values,
        target,
        source,
        columns,
    )
    potential = sum_at_column(parts)
    weighted = (weights[:, :, None] * potential).astype(BF16).reshape(batches * pts, width)

    half = batches * pts // 2
    side = lax.axis_size("z")
    all_weighted = lax.all_gather(weighted[:half], GRID, axis=0, tiled=True)
    line = to_everyone(weighted[half:], "y")
    lined_basis = own_basis.reshape(lax.axis_size("y"), side, CAPB * BLK, batches * pts)
    offsets = [0]
    for step in range(1, side // 2 + 1):
        offsets += [side - step, step]
    lines = (lax.axis_index("z") + jnp.array(offsets[:side], jnp.int32)) & (side - 1)
    ahead = [(i, (i + 1) % side) for i in range(side)]
    behind = [(i, (i - 1) % side) for i in range(side)]
    up = down = line
    came = [line]
    fock = None
    for step in range(1, side // 2 + 1):
        up = lax.ppermute(up, "z", ahead)
        if step < side - step:
            down = lax.ppermute(down, "z", behind)
        fock = fock_from_lines(pick, lines, max(0, 2 * step - 3), lined_basis, came, fock, held)
        if step < side - step:
            up, down, fock = lax.optimization_barrier((up, down, fock))
            came = [up, down]
        else:
            fock = fock_from_gather(
                pick, own_basis, all_weighted.reshape(owners, half, width), fock
            )
            fock = fock_from_lines(pick, lines, 2 * step - 1, lined_basis, [up], fock, held)
    return fock.reshape(held * BLK, width)


def solution(mesh):
    columns = mesh.shape["col"]
    side = math.isqrt(mesh.shape["grid"])
    planes = Mesh(mesh.devices.reshape(-1, side, columns), (*GRID, "col"))
    return jax.shard_map(
        on_device,
        mesh=planes,
        in_specs=(
            P(GRID, "col"),
            P(None, GRID),
            P(GRID),
            P(None, "col"),
            P("col"),
            P(GRID, None, None),
            P(GRID, None),
            P(),
            P(GRID, "col"),
            P(GRID, "col"),
        ),
        out_specs=P(GRID, "col"),
        check_vma=False,
    )
```

```python
import functools
import math

import jax
import jax.numpy as jnp
from jax import lax
from jax.experimental import pallas as pl
from jax.experimental.pallas import tpu as pltpu
from jax.sharding import Mesh
from jax.sharding import PartitionSpec as P

BLK = 128
CAPB = 2
PARAMS = 4
CHUNK = 512
STEP_OWNERS = 4
SCALE_ROWS = 16
PARTS = 2
GRID = ("y", "z")
quad_nodes = 8
F32 = jnp.float32
BF16 = jnp.bfloat16


def call(kernel, name, flops=0, **kwargs):
    return pl.pallas_call(
        kernel,
        name=name,
        compiler_params=pltpu.CompilerParams(
            dimension_semantics=("arbitrary",) * len(kwargs["grid_spec"].grid),
        ),
        cost_estimate=pl.CostEstimate(flops=flops, transcendentals=0, bytes_accessed=0),
        **kwargs,
    )


def line_basis_kernel(rows_at, listed, gathered, points, out, spots, *, batches, slots):
    place = pl.program_id(0)
    for row in range(3 * batches):
        spots[row] = jnp.broadcast_to(points[0, :, row : row + 1], spots.shape[1:])

    def one_slot(slot, carry):
        row = rows_at[place * slots + slot]
        lanes = pl.ds(pl.multiple_of(slot * BLK, BLK), BLK)
        for batch in range(batches):
            keep = listed[(place * slots + slot) * batches + batch]
            here = (0, slice(batch * BLK, (batch + 1) * BLK), lanes)

            @pl.when(keep > 0)
            def _():
                squared = None
                for axis in range(3):
                    delta = spots[axis * batches + batch] - gathered[pl.ds(row + axis, 1), :]
                    squared = delta * delta if squared is None else squared + delta * delta
                out[here] = jnp.exp(-gathered[pl.ds(row + 3, 1), :] * squared).astype(BF16)

            @pl.when(keep == 0)
            def _():
                out[here] = jnp.zeros((BLK, BLK), BF16)

        return carry

    lax.fori_loop(0, slots, one_slot, 0)


def line_basis(rows_at, listed, gathered, points_t, batches):
    places, pts, rows = points_t.shape
    slots = rows_at.shape[0] // places
    return call(
        functools.partial(line_basis_kernel, batches=batches, slots=slots),
        "line_basis",
        flops=places * batches * pts * slots * BLK * 50,
        grid_spec=pltpu.PrefetchScalarGridSpec(
            num_scalar_prefetch=2,
            grid=(places,),
            in_specs=[
                pl.BlockSpec(gathered.shape, lambda i, *_: (0, 0)),
                pl.BlockSpec((1, pts, rows), lambda i, *_: (i, 0, 0)),
            ],
            out_specs=pl.BlockSpec((1, batches * pts, slots * BLK), lambda i, *_: (i, 0, 0)),
            scratch_shapes=[pltpu.VMEM((rows, pts, BLK), F32)],
        ),
        out_shape=jax.ShapeDtypeStruct((places, batches * pts, slots * BLK), BF16),
    )(rows_at, listed, gathered, points_t)


def line_field_kernel(tiles_at, tiles, basis, out, rows, *, slots):
    place = pl.program_id(0)
    for slot in range(slots):
        rows[slot * BLK : (slot + 1) * BLK, :] = tiles[tiles_at[place * slots + slot]]
    out[0] = jnp.dot(basis[0], rows[...], preferred_element_type=F32)


def line_field(tiles_at, tiles, basis, part, parts):
    places, points, functions = basis.shape
    count, _, width = tiles.shape
    points //= parts
    return call(
        functools.partial(line_field_kernel, slots=functions // BLK),
        "line_field",
        flops=2 * places * points * functions * width,
        grid_spec=pltpu.PrefetchScalarGridSpec(
            num_scalar_prefetch=1,
            grid=(places,),
            in_specs=[
                pl.BlockSpec((count, BLK, width), lambda i, *_: (0, 0, 0)),
                pl.BlockSpec((1, points, functions), lambda i, *_: (i, part, 0)),
            ],
            out_specs=pl.BlockSpec((1, points, width), lambda i, *_: (i, 0, 0)),
            scratch_shapes=[pltpu.VMEM((functions, width), BF16)],
        ),
        out_shape=jax.ShapeDtypeStruct((places, points, width), F32),
    )(tiles_at, tiles, basis)


def one_hot(columns, rows):
    spot = lax.broadcasted_iota(jnp.int32, (rows, columns.shape[1]), 0)
    return jnp.where(spot == columns, 1.0, 0.0).astype(BF16)


def rejoin(picked):
    return picked[0:4] + picked[4:8] + picked[8:12]


def pair_kernel(target, source, window, local, points, out, spots):
    @pl.when(pl.program_id(1) == 0)
    def _():
        for axis in range(3):
            spots[axis] = jnp.broadcast_to(points[0, :, axis : axis + 1], spots.shape[1:])

    target_par = rejoin(
        jnp.dot(window[...], one_hot(target[0], window.shape[1]), preferred_element_type=F32)
    )
    source_par = rejoin(
        jnp.dot(local[...], one_hot(source[0], local.shape[1]), preferred_element_type=F32)
    )
    target_exp, source_exp = target_par[3:4], source_par[3:4]
    joined = target_exp + source_exp
    separation = jnp.zeros_like(joined)
    centres = []
    for axis in range(3):
        here, there = target_par[axis : axis + 1], source_par[axis : axis + 1]
        offset = here - there
        separation = separation + offset * offset
        centres.append((target_exp * here + source_exp * there) / joined)
    prefactor = 2.0 * math.pi / joined * jnp.exp(-target_exp * source_exp / joined * separation)
    lanes = spots.shape[2]
    for first in range(0, joined.shape[1], lanes):
        part = slice(first, first + lanes)
        spread = None
        for axis in range(3):
            delta = spots[axis] - centres[axis][:, part]
            spread = delta * delta if spread is None else spread + delta * delta
        argument = joined[:, part] * spread
        summed = jnp.zeros_like(argument)
        for quad_node in range(quad_nodes):
            node_spot = (quad_node + 0.5) / quad_nodes
            summed = summed + jnp.exp(-argument * (node_spot * node_spot))
        out[0, :, part] = prefactor[:, part] * (summed / quad_nodes)


def pair_values(target, source, window, local, points_t):
    batches, _, pairs = target.shape
    pts = points_t.shape[1]
    return call(
        pair_kernel,
        "pair_values",
        flops=batches * pairs * pts * 400,
        grid_spec=pltpu.PrefetchScalarGridSpec(
            num_scalar_prefetch=0,
            grid=(batches, pairs // CHUNK),
            in_specs=[
                pl.BlockSpec((1, 1, CHUNK), lambda b, n: (b, 0, n)),
                pl.BlockSpec((1, 1, CHUNK), lambda b, n: (b, 0, n)),
                pl.BlockSpec(window.shape, lambda b, n: (0, 0)),
                pl.BlockSpec(local.shape, lambda b, n: (0, 0)),
                pl.BlockSpec((1, pts, 3), lambda b, n: (b, 0, 0)),
            ],
            out_specs=pl.BlockSpec((1, pts, CHUNK), lambda b, n: (b, 0, n)),
            scratch_shapes=[pltpu.VMEM((3, pts, BLK), F32)],
        ),
        out_shape=jax.ShapeDtypeStruct((batches, pts, pairs), F32),
    )(target, source, window, local, points_t)


def potential_kernel(field, values, target, source, out):
    columns, width = out.shape[0], out.shape[3]
    window_count = columns * width
    potential = jnp.zeros((field.shape[1], window_count), F32)
    for first in range(0, values.shape[2], CHUNK):
        part = slice(first, first + CHUNK)
        picked = jnp.dot(field[0], one_hot(source[0, :, part], width), preferred_element_type=F32)
        product = (values[0, :, part] * picked).astype(BF16)
        potential += lax.dot_general(
            product,
            one_hot(target[0, :, part], window_count),
            (((1,), (1,)), ((), ())),
            preferred_element_type=F32,
        )
    for column in range(columns):
        out[column, 0] = potential[:, column * width : (column + 1) * width]


def potential_parts(field, values, target, source, first, columns):
    batches, pts, width = field.shape
    pairs = values.shape[2]
    return call(
        potential_kernel,
        "potential_parts",
        flops=2 * batches * pts * pairs * columns * width,
        grid_spec=pltpu.PrefetchScalarGridSpec(
            num_scalar_prefetch=0,
            grid=(batches,),
            in_specs=[
                pl.BlockSpec((1, pts, width), lambda b: (b, 0, 0)),
                pl.BlockSpec((1, pts, pairs), lambda b: (first + b, 0, 0)),
                pl.BlockSpec((1, 1, pairs), lambda b: (first + b, 0, 0)),
                pl.BlockSpec((1, 1, pairs), lambda b: (first + b, 0, 0)),
            ],
            out_specs=pl.BlockSpec((columns, 1, pts, width), lambda b: (0, b, 0, 0)),
        ),
        out_shape=jax.ShapeDtypeStruct((columns, batches, pts, width), F32),
    )(field, values, target, source)


def owner_basis_kernel(pick, listed, points_at, params, gathered, out, spread_params, *, batches):
    @pl.when(pl.program_id(0) == 0)
    def _():
        for block in range(spread_params.shape[0]):
            for which in range(PARAMS):
                spread_params[block, which] = jnp.broadcast_to(
                    params[block * BLK : (block + 1) * BLK, which : which + 1], (BLK, BLK)
                )

    def one_owner(owner, carry):
        place = pl.program_id(0) * STEP_OWNERS + owner
        for slot in range(CAPB):
            block = pick[place * CAPB + slot]
            for batch in range(batches):
                here = (owner, slice(slot * BLK, (slot + 1) * BLK), slice(batch * BLK, (batch + 1) * BLK))
                keep = listed[(place * CAPB + slot) * batches + batch]

                @pl.when(keep > 0)
                def _():
                    squared = None
                    for axis in range(3):
                        row = points_at[place] + axis * batches + batch
                        delta = gathered[pl.ds(row, 1), :] - spread_params[block, axis]
                        squared = delta * delta if squared is None else squared + delta * delta
                    out[here] = jnp.exp(-spread_params[block, 3] * squared).astype(BF16)

                @pl.when(keep == 0)
                def _():
                    out[here] = jnp.zeros((BLK, BLK), BF16)

        return carry

    lax.fori_loop(0, STEP_OWNERS, one_owner, 0)


def basis_at_owner(pick, listed, points_at, params_t, gathered, batches, pts):
    owners = points_at.shape[0]
    held = params_t.shape[0] // BLK
    return call(
        functools.partial(owner_basis_kernel, batches=batches),
        "basis_at_owner",
        flops=owners * CAPB * BLK * batches * pts * 50,
        grid_spec=pltpu.PrefetchScalarGridSpec(
            num_scalar_prefetch=3,
            grid=(owners // STEP_OWNERS,),
            in_specs=[
                pl.BlockSpec(params_t.shape, lambda i, *_: (0, 0)),
                pl.BlockSpec(gathered.shape, lambda i, *_: (0, 0)),
            ],
            out_specs=pl.BlockSpec((STEP_OWNERS, CAPB * BLK, batches * pts), lambda i, *_: (i, 0, 0)),
            scratch_shapes=[pltpu.VMEM((held, PARAMS, BLK, BLK), F32)],
        ),
        out_shape=jax.ShapeDtypeStruct((owners, CAPB * BLK, batches * pts), BF16),
    )(pick, listed, points_at, params_t, gathered)


def add_rows(out, pick, place, rows):
    for slot in range(CAPB):
        block = pick[place * CAPB + slot]
        out[block] = out[block] + rows[slot * BLK : (slot + 1) * BLK]


def fock_kernel(pick, basis, weighted, *refs):
    out = refs[-1]

    @pl.when(pl.program_id(0) == 0)
    def _():
        out[...] = refs[0][...] if len(refs) > 1 else jnp.zeros_like(out)

    for owner in range(STEP_OWNERS):
        place = pl.program_id(0) * STEP_OWNERS + owner
        add_rows(out, pick, place, jnp.dot(basis[owner], weighted[owner], preferred_element_type=F32))


def fock_at_owner(pick, basis, weighted, part, before, held):
    owners, rows, _ = basis.shape
    _, points, width = weighted.shape
    whole = pl.BlockSpec((held, BLK, width), lambda i, *_: (0, 0, 0))
    return call(
        fock_kernel,
        "fock_at_owner",
        flops=2 * owners * rows * points * width,
        grid_spec=pltpu.PrefetchScalarGridSpec(
            num_scalar_prefetch=1,
            grid=(owners // STEP_OWNERS,),
            in_specs=[
                pl.BlockSpec((STEP_OWNERS, rows, points), lambda i, *_: (i, 0, part)),
                pl.BlockSpec((STEP_OWNERS, points, width), lambda i, *_: (i, 0, 0)),
            ]
            + ([] if before is None else [whole]),
            out_specs=whole,
        ),
        out_shape=jax.ShapeDtypeStruct((held, BLK, width), F32),
        input_output_aliases={} if before is None else {3: 0},
    )(pick, basis, weighted, *([] if before is None else [before]))


def to_everyone(value, axis):
    devices = lax.axis_size(axis)
    return lax.all_to_all(
        jnp.broadcast_to(value[None], (devices, *value.shape)), axis, 0, 0, tiled=True
    )


def in_parts(values):
    high = lax.reduce_precision(values, 8, 7)
    middle = lax.reduce_precision(values - high, 8, 7)
    low = values - high - middle
    parts = jnp.concatenate([high, middle, low, jnp.zeros_like(low)], axis=0)
    return parts.astype(BF16)


def sum_at_column(parts):
    columns, batches, pts, width = parts.shape
    largest = jnp.max(jnp.abs(parts), axis=(0, 2, 3))
    power = jnp.clip(13.0 - jnp.ceil(jnp.log2(largest)), -100.0, 100.0)
    scaled = (parts * jnp.exp2(power)[None, :, None, None]).astype(jnp.float16)
    tail = jnp.broadcast_to(
        power[None, :, None, None], (columns, batches, SCALE_ROWS, width)
    ).astype(jnp.float16)
    got = lax.all_to_all(
        jnp.concatenate([scaled, tail], axis=2), "col", split_axis=0, concat_axis=0, tiled=True
    )
    factor = jnp.exp2(-got[:, :, pts : pts + 1, 0:1].astype(F32))
    return jnp.sum(got[:, :, :pts].astype(F32) * factor, axis=0)


def slots_of(lists, base, held, batches):
    spot = lists - base
    owned = (spot >= 0) & (spot < held)
    lowest = jnp.min(jnp.where(owned, spot, held), axis=-1)
    highest = jnp.max(jnp.where(owned, spot, -1), axis=-1)
    ends = jnp.stack([lowest, highest], axis=-1)
    pick = jnp.where((highest >= 0)[..., None], ends, 0).astype(jnp.int32)
    hit = owned[..., None, :] & (spot[..., None, :] == ends[..., None])
    hit = hit & ((lowest != highest)[..., None] | (jnp.arange(CAPB) == 0))[..., None]
    listed = jnp.any(hit.reshape(*hit.shape[:-1], batches, -1), axis=-1)
    return pick, listed.astype(jnp.int32)


def on_device(
    density,
    row_centers,
    row_exps,
    win_centers,
    win_exps,
    points,
    weights,
    sig_blocks,
    pair_target,
    pair_source,
):
    lines, side = lax.axis_size("y"), lax.axis_size("z")
    owners = lines * side
    columns = lax.axis_size("col")
    line, place, column = lax.axis_index("y"), lax.axis_index("z"), lax.axis_index("col")
    held = row_exps.shape[0] // BLK
    width = density.shape[1]
    batches, _, pts = points.shape

    tiles = lax.all_gather(density, "z", axis=0, tiled=True).reshape(side * held, BLK, width)

    own_params = jnp.concatenate([row_centers, row_exps[None, :]], axis=0)
    own_blocks = own_params.reshape(PARAMS, held, BLK).transpose(1, 0, 2).reshape(columns, -1, BLK)
    block_rows = own_blocks.shape[1]
    own_points = points.transpose(1, 0, 2).reshape(3 * batches, pts)
    line_points = to_everyone(own_points, "y")
    point_rows = own_points.shape[0]
    shared = jnp.concatenate(
        [
            lax.dynamic_index_in_dim(own_blocks, column, 0, keepdims=False),
            lax.dynamic_index_in_dim(line_points, column, 0, keepdims=False),
        ],
        axis=0,
    )
    shared = to_everyone(shared, "z").reshape(-1, BLK)
    local_window = jnp.concatenate([win_centers, win_exps[None, :]], axis=0)
    spare = jnp.zeros_like(local_window)
    gathered = to_everyone(jnp.concatenate([shared, local_window, spare], axis=0), "col")
    rows_each = gathered.shape[1]
    whole_window = gathered[:, shared.shape[0] : shared.shape[0] + PARAMS]
    whole_window = whole_window.transpose(1, 0, 2).reshape(PARAMS, -1)
    gathered = gathered.reshape(-1, BLK)

    lists = sig_blocks.reshape(lines, side, -1)
    rows_of_place = block_rows + point_rows
    line_lists = lax.dynamic_index_in_dim(lists, place, 1, keepdims=True)
    base = (line * side + jnp.arange(side, dtype=jnp.int32)) * held
    line_pick, line_listed = slots_of(line_lists, base[None, :, None], held, batches)
    tiles_at = line_pick + (jnp.arange(side, dtype=jnp.int32) * held)[None, :, None]
    blocks_each = held // columns
    rows_at = (
        line_pick // blocks_each * rows_each
        + (jnp.arange(side, dtype=jnp.int32) * rows_of_place)[None, :, None]
        + line_pick % blocks_each * PARAMS
    )
    my_base = (line * side + place) * held
    pick, listed = slots_of(lists.reshape(owners, -1), my_base, held, batches)
    pick, listed = pick.reshape(-1), listed.reshape(-1)
    points_at = (
        jnp.arange(lines, dtype=jnp.int32)[:, None] * rows_each
        + jnp.arange(side, dtype=jnp.int32)[None, :] * rows_of_place
        + block_rows
    ).reshape(-1)

    points_t = points.transpose(0, 2, 1)
    target = pair_target[:, None, :]
    source = pair_source[:, None, :]
    basis = line_basis(
        rows_at.reshape(-1),
        line_listed.reshape(-1),
        gathered,
        line_points.transpose(0, 2, 1),
        batches,
    )
    values = pair_values(target, source, in_parts(whole_window), in_parts(local_window), points_t)
    basis, values = lax.optimization_barrier((basis, values))

    together = batches // PARTS
    weighted = []
    for part in range(PARTS):
        share = line_field(tiles_at.reshape(-1), tiles, basis, part, PARTS)
        field = lax.psum_scatter(
            share.reshape(-1, width), "y", scatter_dimension=0, tiled=True
        ).astype(BF16)
        parts = potential_parts(
            field.reshape(together, pts, width), values, target, source, part * together, columns
        )
        potential = sum_at_column(parts)
        scale = weights[part * together : (part + 1) * together, :, None]
        weighted.append((scale * potential).astype(BF16).reshape(together * pts, width))

    everyone = [lax.all_gather(value, GRID, axis=0, tiled=True) for value in weighted]
    gathered, weighted = lax.optimization_barrier((gathered, weighted[-1]))
    own_basis = basis_at_owner(pick, listed, points_at, own_params.T, gathered, batches, pts)
    fock = None
    for part, value in enumerate(everyone):
        value = value.reshape(owners, together * pts, width)
        fock = fock_at_owner(pick, own_basis, value, part, fock, held)
    return fock.reshape(held * BLK, width)


def solution(mesh):
    columns = mesh.shape["col"]
    side = math.isqrt(mesh.shape["grid"])
    planes = Mesh(mesh.devices.reshape(-1, side, columns), (*GRID, "col"))
    return jax.shard_map(
        on_device,
        mesh=planes,
        in_specs=(
            P(GRID, "col"),
            P(None, GRID),
            P(GRID),
            P(None, "col"),
            P("col"),
            P(GRID, None, None),
            P(GRID, None),
            P(),
            P(GRID, "col"),
            P(GRID, "col"),
        ),
        out_specs=P(GRID, "col"),
        check_vma=False,
    )
```

```python
import functools
import math

import jax
import jax.numpy as jnp
from jax import lax
from jax.experimental import pallas as pl
from jax.experimental.pallas import tpu as pltpu
from jax.sharding import Mesh
from jax.sharding import PartitionSpec as P

BLK = 128
CAPB = 2
PARAMS = 4
CHUNK = 512
STEP_OWNERS = 4
SCALE_ROWS = 16
STEP_GATHERED = 16
STEP_PLACES = 2
GRID = ("y", "z")
quad_nodes = 8
F32 = jnp.float32
BF16 = jnp.bfloat16


def call(kernel, name, flops=0, **kwargs):
    return pl.pallas_call(
        kernel,
        name=name,
        compiler_params=pltpu.CompilerParams(
            dimension_semantics=("arbitrary",) * len(kwargs["grid_spec"].grid),
        ),
        cost_estimate=pl.CostEstimate(flops=flops, transcendentals=0, bytes_accessed=0),
        **kwargs,
    )


def line_basis_kernel(rows_at, listed, gathered, points, out, spots, *, batches, slots):
    place = pl.program_id(0)
    for row in range(3 * batches):
        spots[row] = jnp.broadcast_to(points[0, :, row : row + 1], spots.shape[1:])

    def one_slot(slot, carry):
        row = rows_at[place * slots + slot]
        lanes = pl.ds(pl.multiple_of(slot * BLK, BLK), BLK)
        for batch in range(batches):
            keep = listed[(place * slots + slot) * batches + batch]
            here = (0, slice(batch * BLK, (batch + 1) * BLK), lanes)

            @pl.when(keep > 0)
            def _():
                squared = None
                for axis in range(3):
                    delta = spots[axis * batches + batch] - gathered[pl.ds(row + axis, 1), :]
                    squared = delta * delta if squared is None else squared + delta * delta
                out[here] = jnp.exp(-gathered[pl.ds(row + 3, 1), :] * squared).astype(BF16)

            @pl.when(keep == 0)
            def _():
                out[here] = jnp.zeros((BLK, BLK), BF16)

        return carry

    lax.fori_loop(0, slots, one_slot, 0)


def line_basis(rows_at, listed, gathered, points_t, batches):
    places, pts, rows = points_t.shape
    slots = rows_at.shape[0] // places
    return call(
        functools.partial(line_basis_kernel, batches=batches, slots=slots),
        "line_basis",
        flops=places * batches * pts * slots * BLK * 50,
        grid_spec=pltpu.PrefetchScalarGridSpec(
            num_scalar_prefetch=2,
            grid=(places,),
            in_specs=[
                pl.BlockSpec(gathered.shape, lambda i, *_: (0, 0)),
                pl.BlockSpec((1, pts, rows), lambda i, *_: (i, 0, 0)),
            ],
            out_specs=pl.BlockSpec((1, batches * pts, slots * BLK), lambda i, *_: (i, 0, 0)),
            scratch_shapes=[pltpu.VMEM((rows, pts, BLK), F32)],
        ),
        out_shape=jax.ShapeDtypeStruct((places, batches * pts, slots * BLK), BF16),
    )(rows_at, listed, gathered, points_t)


def line_field_kernel(tiles_at, tiles, basis, out, rows, *, slots):
    for place in range(out.shape[0]):
        first = (pl.program_id(0) * out.shape[0] + place) * slots
        for slot in range(slots):
            rows[place, slot * BLK : (slot + 1) * BLK, :] = tiles[tiles_at[first + slot]]
        out[place] = jnp.dot(basis[place], rows[place], preferred_element_type=F32)


def line_field(tiles_at, tiles, basis):
    places, points, functions = basis.shape
    count, _, width = tiles.shape
    step = min(STEP_PLACES, places)
    return call(
        functools.partial(line_field_kernel, slots=functions // BLK),
        "line_field",
        flops=2 * places * points * functions * width,
        grid_spec=pltpu.PrefetchScalarGridSpec(
            num_scalar_prefetch=1,
            grid=(places // step,),
            in_specs=[
                pl.BlockSpec((count, BLK, width), lambda i, *_: (0, 0, 0)),
                pl.BlockSpec((step, points, functions), lambda i, *_: (i, 0, 0)),
            ],
            out_specs=pl.BlockSpec((step, points, width), lambda i, *_: (i, 0, 0)),
            scratch_shapes=[pltpu.VMEM((step, functions, width), BF16)],
        ),
        out_shape=jax.ShapeDtypeStruct((places, points, width), F32),
    )(tiles_at, tiles, basis)


def one_hot(columns, rows):
    spot = lax.broadcasted_iota(jnp.int32, (rows, columns.shape[1]), 0)
    return jnp.where(spot == columns, 1.0, 0.0).astype(BF16)


def rejoin(picked):
    return picked[0:4] + picked[4:8] + picked[8:12]


def pair_kernel(target, source, window, local, points, out, spots):
    @pl.when(pl.program_id(1) == 0)
    def _():
        for axis in range(3):
            spots[axis] = jnp.broadcast_to(points[0, :, axis : axis + 1], spots.shape[1:])

    target_par = rejoin(
        jnp.dot(window[...], one_hot(target[0], window.shape[1]), preferred_element_type=F32)
    )
    source_par = rejoin(
        jnp.dot(local[...], one_hot(source[0], local.shape[1]), preferred_element_type=F32)
    )
    target_exp, source_exp = target_par[3:4], source_par[3:4]
    joined = target_exp + source_exp
    separation = jnp.zeros_like(joined)
    centres = []
    for axis in range(3):
        here, there = target_par[axis : axis + 1], source_par[axis : axis + 1]
        offset = here - there
        separation = separation + offset * offset
        centres.append((target_exp * here + source_exp * there) / joined)
    prefactor = 2.0 * math.pi / joined * jnp.exp(-target_exp * source_exp / joined * separation)
    lanes = spots.shape[2]
    for first in range(0, joined.shape[1], lanes):
        part = slice(first, first + lanes)
        spread = None
        for axis in range(3):
            delta = spots[axis] - centres[axis][:, part]
            spread = delta * delta if spread is None else spread + delta * delta
        argument = joined[:, part] * spread
        summed = jnp.zeros_like(argument)
        for quad_node in range(quad_nodes):
            node_spot = (quad_node + 0.5) / quad_nodes
            summed = summed + jnp.exp(-argument * (node_spot * node_spot))
        out[0, :, part] = prefactor[:, part] * (summed / quad_nodes)


def pair_values(target, source, window, local, points_t):
    batches, _, pairs = target.shape
    pts = points_t.shape[1]
    return call(
        pair_kernel,
        "pair_values",
        flops=batches * pairs * pts * 400,
        grid_spec=pltpu.PrefetchScalarGridSpec(
            num_scalar_prefetch=0,
            grid=(batches, pairs // CHUNK),
            in_specs=[
                pl.BlockSpec((1, 1, CHUNK), lambda b, n: (b, 0, n)),
                pl.BlockSpec((1, 1, CHUNK), lambda b, n: (b, 0, n)),
                pl.BlockSpec(window.shape, lambda b, n: (0, 0)),
                pl.BlockSpec(local.shape, lambda b, n: (0, 0)),
                pl.BlockSpec((1, pts, 3), lambda b, n: (b, 0, 0)),
            ],
            out_specs=pl.BlockSpec((1, pts, CHUNK), lambda b, n: (b, 0, n)),
            scratch_shapes=[pltpu.VMEM((3, pts, BLK), F32)],
        ),
        out_shape=jax.ShapeDtypeStruct((batches, pts, pairs), F32),
    )(target, source, window, local, points_t)


def potential_kernel(field, values, target, source, out, largest):
    columns, width = out.shape[0], out.shape[3]
    window_count = columns * width
    rounded = field[0].astype(BF16)
    potential = jnp.zeros((field.shape[1], window_count), F32)
    for first in range(0, values.shape[2], CHUNK):
        part = slice(first, first + CHUNK)
        picked = jnp.dot(rounded, one_hot(source[0, :, part], width), preferred_element_type=F32)
        product = (values[0, :, part] * picked).astype(BF16)
        potential += lax.dot_general(
            product,
            one_hot(target[0, :, part], window_count),
            (((1,), (1,)), ((), ())),
            preferred_element_type=F32,
        )
    for column in range(columns):
        out[column, 0] = potential[:, column * width : (column + 1) * width]
    largest[0] = jnp.broadcast_to(jnp.max(jnp.abs(potential), keepdims=True), largest.shape[1:])


def potential_parts(field, values, target, source, columns):
    batches, pts, width = field.shape
    pairs = values.shape[2]
    return call(
        potential_kernel,
        "potential_parts",
        flops=2 * batches * pts * pairs * columns * width,
        grid_spec=pltpu.PrefetchScalarGridSpec(
            num_scalar_prefetch=0,
            grid=(batches,),
            in_specs=[
                pl.BlockSpec((1, pts, width), lambda b: (b, 0, 0)),
                pl.BlockSpec((1, pts, pairs), lambda b: (b, 0, 0)),
                pl.BlockSpec((1, 1, pairs), lambda b: (b, 0, 0)),
                pl.BlockSpec((1, 1, pairs), lambda b: (b, 0, 0)),
            ],
            out_specs=[
                pl.BlockSpec((columns, 1, pts, width), lambda b: (0, b, 0, 0)),
                pl.BlockSpec((1, 8, BLK), lambda b: (b, 0, 0)),
            ],
        ),
        out_shape=[
            jax.ShapeDtypeStruct((columns, batches, pts, width), F32),
            jax.ShapeDtypeStruct((batches, 8, BLK), F32),
        ],
    )(field, values, target, source)


def owner_basis_kernel(pick, listed, points_at, params, gathered, out, spread_params, *, batches):
    @pl.when(pl.program_id(0) == 0)
    def _():
        for block in range(spread_params.shape[0]):
            for which in range(PARAMS):
                spread_params[block, which] = jnp.broadcast_to(
                    params[block * BLK : (block + 1) * BLK, which : which + 1], (BLK, BLK)
                )

    def one_owner(owner, carry):
        place = pl.program_id(0) * STEP_OWNERS + owner
        for slot in range(CAPB):
            block = pick[place * CAPB + slot]
            for batch in range(batches):
                here = (owner, slice(slot * BLK, (slot + 1) * BLK), slice(batch * BLK, (batch + 1) * BLK))
                keep = listed[(place * CAPB + slot) * batches + batch]

                @pl.when(keep > 0)
                def _():
                    squared = None
                    for axis in range(3):
                        row = points_at[place] + axis * batches + batch
                        delta = gathered[pl.ds(row, 1), :] - spread_params[block, axis]
                        squared = delta * delta if squared is None else squared + delta * delta
                    out[here] = jnp.exp(-spread_params[block, 3] * squared).astype(BF16)

                @pl.when(keep == 0)
                def _():
                    out[here] = jnp.zeros((BLK, BLK), BF16)

        return carry

    lax.fori_loop(0, STEP_OWNERS, one_owner, 0)


def basis_at_owner(pick, listed, points_at, params_t, gathered, batches, pts):
    owners = points_at.shape[0]
    held = params_t.shape[0] // BLK
    return call(
        functools.partial(owner_basis_kernel, batches=batches),
        "basis_at_owner",
        flops=owners * CAPB * BLK * batches * pts * 50,
        grid_spec=pltpu.PrefetchScalarGridSpec(
            num_scalar_prefetch=3,
            grid=(owners // STEP_OWNERS,),
            in_specs=[
                pl.BlockSpec(params_t.shape, lambda i, *_: (0, 0)),
                pl.BlockSpec(gathered.shape, lambda i, *_: (0, 0)),
            ],
            out_specs=pl.BlockSpec((STEP_OWNERS, CAPB * BLK, batches * pts), lambda i, *_: (i, 0, 0)),
            scratch_shapes=[pltpu.VMEM((held, PARAMS, BLK, BLK), F32)],
        ),
        out_shape=jax.ShapeDtypeStruct((owners, CAPB * BLK, batches * pts), BF16),
    )(pick, listed, points_at, params_t, gathered)


def add_rows(out, pick, place, rows):
    for slot in range(CAPB):
        block = pick[place * CAPB + slot]
        out[block] = out[block] + rows[slot * BLK : (slot + 1) * BLK]


def fock_kernel(pick, basis, weighted, out):
    @pl.when(pl.program_id(0) == 0)
    def _():
        out[...] = jnp.zeros_like(out)

    for owner in range(basis.shape[0]):
        place = pl.program_id(0) * basis.shape[0] + owner
        add_rows(out, pick, place, jnp.dot(basis[owner], weighted[owner], preferred_element_type=F32))


def fock_at_owner(pick, basis, weighted, held):
    owners, rows, points = basis.shape
    width = weighted.shape[2]
    step = min(STEP_GATHERED, owners)
    return call(
        fock_kernel,
        "fock_at_owner",
        flops=2 * owners * rows * points * width,
        grid_spec=pltpu.PrefetchScalarGridSpec(
            num_scalar_prefetch=1,
            grid=(owners // step,),
            in_specs=[
                pl.BlockSpec((step, rows, points), lambda i, *_: (i, 0, 0)),
                pl.BlockSpec((step, points, width), lambda i, *_: (i, 0, 0)),
            ],
            out_specs=pl.BlockSpec((held, BLK, width), lambda i, *_: (0, 0, 0)),
        ),
        out_shape=jax.ShapeDtypeStruct((held, BLK, width), F32),
    )(pick, basis, weighted)


def to_everyone(value, axis):
    devices = lax.axis_size(axis)
    return lax.all_to_all(
        jnp.broadcast_to(value[None], (devices, *value.shape)), axis, 0, 0, tiled=True
    )


def in_parts(values):
    high = lax.reduce_precision(values, 8, 7)
    middle = lax.reduce_precision(values - high, 8, 7)
    low = values - high - middle
    parts = jnp.concatenate([high, middle, low, jnp.zeros_like(low)], axis=0)
    return parts.astype(BF16)


def sum_at_column(parts, largest):
    columns, batches, pts, width = parts.shape
    power = jnp.clip(13.0 - jnp.ceil(jnp.log2(largest)), -100.0, 100.0)
    scaled = (parts * jnp.exp2(power)[None, :, None, None]).astype(jnp.float16)
    tail = jnp.broadcast_to(
        power[None, :, None, None], (columns, batches, SCALE_ROWS, width)
    ).astype(jnp.float16)
    got = lax.all_to_all(
        jnp.concatenate([scaled, tail], axis=2), "col", split_axis=0, concat_axis=0, tiled=True
    )
    factor = jnp.exp2(-got[:, :, pts : pts + 1, 0:1].astype(F32))
    return jnp.sum(got[:, :, :pts].astype(F32) * factor, axis=0)


def slots_of(lists, base, held, batches):
    spot = lists - base
    owned = (spot >= 0) & (spot < held)
    lowest = jnp.min(jnp.where(owned, spot, held), axis=-1)
    highest = jnp.max(jnp.where(owned, spot, -1), axis=-1)
    ends = jnp.stack([lowest, highest], axis=-1)
    pick = jnp.where((highest >= 0)[..., None], ends, 0).astype(jnp.int32)
    hit = owned[..., None, :] & (spot[..., None, :] == ends[..., None])
    hit = hit & ((lowest != highest)[..., None] | (jnp.arange(CAPB) == 0))[..., None]
    listed = jnp.any(hit.reshape(*hit.shape[:-1], batches, -1), axis=-1)
    return pick, listed.astype(jnp.int32)


def on_device(
    density,
    row_centers,
    row_exps,
    win_centers,
    win_exps,
    points,
    weights,
    sig_blocks,
    pair_target,
    pair_source,
):
    lines, side = lax.axis_size("y"), lax.axis_size("z")
    owners = lines * side
    columns = lax.axis_size("col")
    line, place, column = lax.axis_index("y"), lax.axis_index("z"), lax.axis_index("col")
    held = row_exps.shape[0] // BLK
    width = density.shape[1]
    batches, _, pts = points.shape

    tiles = lax.all_gather(density, "z", axis=0, tiled=True).reshape(side * held, BLK, width)

    own_params = jnp.concatenate([row_centers, row_exps[None, :]], axis=0)
    own_blocks = own_params.reshape(PARAMS, held, BLK).transpose(1, 0, 2).reshape(columns, -1, BLK)
    block_rows = own_blocks.shape[1]
    own_points = points.transpose(1, 0, 2).reshape(3 * batches, pts)
    line_points = to_everyone(own_points, "y")
    point_rows = own_points.shape[0]
    shared = jnp.concatenate(
        [
            lax.dynamic_index_in_dim(own_blocks, column, 0, keepdims=False),
            lax.dynamic_index_in_dim(line_points, column, 0, keepdims=False),
        ],
        axis=0,
    )
    shared = to_everyone(shared, "z").reshape(-1, BLK)
    local_window = jnp.concatenate([win_centers, win_exps[None, :]], axis=0)
    spare = jnp.zeros_like(local_window)
    gathered = to_everyone(jnp.concatenate([shared, local_window, spare], axis=0), "col")
    rows_each = gathered.shape[1]
    whole_window = gathered[:, shared.shape[0] : shared.shape[0] + PARAMS]
    whole_window = whole_window.transpose(1, 0, 2).reshape(PARAMS, -1)
    gathered = gathered.reshape(-1, BLK)

    lists = sig_blocks.reshape(lines, side, -1)
    rows_of_place = block_rows + point_rows
    line_lists = lax.dynamic_index_in_dim(lists, place, 1, keepdims=True)
    base = (line * side + jnp.arange(side, dtype=jnp.int32)) * held
    line_pick, line_listed = slots_of(line_lists, base[None, :, None], held, batches)
    tiles_at = line_pick + (jnp.arange(side, dtype=jnp.int32) * held)[None, :, None]
    blocks_each = held // columns
    rows_at = (
        line_pick // blocks_each * rows_each
        + (jnp.arange(side, dtype=jnp.int32) * rows_of_place)[None, :, None]
        + line_pick % blocks_each * PARAMS
    )
    my_base = (line * side + place) * held
    pick, listed = slots_of(lists.reshape(owners, -1), my_base, held, batches)
    pick, listed = pick.reshape(-1), listed.reshape(-1)
    points_at = (
        jnp.arange(lines, dtype=jnp.int32)[:, None] * rows_each
        + jnp.arange(side, dtype=jnp.int32)[None, :] * rows_of_place
        + block_rows
    ).reshape(-1)

    points_t = points.transpose(0, 2, 1)
    target = pair_target[:, None, :]
    source = pair_source[:, None, :]
    basis = line_basis(
        rows_at.reshape(-1),
        line_listed.reshape(-1),
        gathered,
        line_points.transpose(0, 2, 1),
        batches,
    )
    share = line_field(tiles_at.reshape(-1), tiles, basis)
    share, local_window, whole_window = lax.optimization_barrier(
        (share, local_window, whole_window)
    )
    field = lax.psum_scatter(share.reshape(-1, width), "y", scatter_dimension=0, tiled=True)
    values = pair_values(target, source, in_parts(whole_window), in_parts(local_window), points_t)
    parts, largest = potential_parts(
        field.reshape(batches, pts, width), values, target, source, columns
    )
    potential = sum_at_column(parts, largest[:, 0, 0])
    weighted = (weights[:, :, None] * potential).astype(BF16).reshape(batches * pts, width)

    all_weighted = lax.all_gather(weighted, GRID, axis=0, tiled=True)
    gathered, weighted = lax.optimization_barrier((gathered, weighted))
    own_basis = basis_at_owner(pick, listed, points_at, own_params.T, gathered, batches, pts)
    fock = fock_at_owner(
        pick, own_basis, all_weighted.reshape(owners, batches * pts, width), held
    )
    return fock.reshape(held * BLK, width)


def solution(mesh):
    columns = mesh.shape["col"]
    side = math.isqrt(mesh.shape["grid"])
    planes = Mesh(mesh.devices.reshape(-1, side, columns), (*GRID, "col"))
    return jax.shard_map(
        on_device,
        mesh=planes,
        in_specs=(
            P(GRID, "col"),
            P(None, GRID),
            P(GRID),
            P(None, "col"),
            P("col"),
            P(GRID, None, None),
            P(GRID, None),
            P(),
            P(GRID, "col"),
            P(GRID, "col"),
        ),
        out_specs=P(GRID, "col"),
        check_vma=False,
    )
```

```python
import functools
import math

import jax
import jax.numpy as jnp
from jax import lax
from jax.experimental import pallas as pl
from jax.experimental.pallas import tpu as pltpu
from jax.sharding import Mesh
from jax.sharding import PartitionSpec as P

BLK = 128
CAPB = 2
PARAMS = 4
CHUNK = 512
STEP_OWNERS = 4
SCALE_ROWS = 16
STEP_GATHERED = 16
STEP_PLACES = 2
PARTS = 2
GRID = ("y", "z")
quad_nodes = 8
F32 = jnp.float32
BF16 = jnp.bfloat16


def call(kernel, name, flops=0, **kwargs):
    return pl.pallas_call(
        kernel,
        name=name,
        compiler_params=pltpu.CompilerParams(
            dimension_semantics=("arbitrary",) * len(kwargs["grid_spec"].grid),
        ),
        cost_estimate=pl.CostEstimate(flops=flops, transcendentals=0, bytes_accessed=0),
        **kwargs,
    )


def line_basis_kernel(rows_at, listed, gathered, points, out, spots, *, batches, slots):
    place = pl.program_id(0)
    for row in range(3 * batches):
        spots[row] = jnp.broadcast_to(points[0, :, row : row + 1], spots.shape[1:])

    def one_slot(slot, carry):
        row = rows_at[place * slots + slot]
        lanes = pl.ds(pl.multiple_of(slot * BLK, BLK), BLK)
        for batch in range(batches):
            keep = listed[(place * slots + slot) * batches + batch]
            here = (0, slice(batch * BLK, (batch + 1) * BLK), lanes)

            @pl.when(keep > 0)
            def _():
                squared = None
                for axis in range(3):
                    delta = spots[axis * batches + batch] - gathered[pl.ds(row + axis, 1), :]
                    squared = delta * delta if squared is None else squared + delta * delta
                out[here] = jnp.exp(-gathered[pl.ds(row + 3, 1), :] * squared).astype(BF16)

            @pl.when(keep == 0)
            def _():
                out[here] = jnp.zeros((BLK, BLK), BF16)

        return carry

    lax.fori_loop(0, slots, one_slot, 0)


def line_basis(rows_at, listed, gathered, points_t, batches):
    places, pts, rows = points_t.shape
    slots = rows_at.shape[0] // places
    return call(
        functools.partial(line_basis_kernel, batches=batches, slots=slots),
        "line_basis",
        flops=places * batches * pts * slots * BLK * 50,
        grid_spec=pltpu.PrefetchScalarGridSpec(
            num_scalar_prefetch=2,
            grid=(places,),
            in_specs=[
                pl.BlockSpec(gathered.shape, lambda i, *_: (0, 0)),
                pl.BlockSpec((1, pts, rows), lambda i, *_: (i, 0, 0)),
            ],
            out_specs=pl.BlockSpec((1, batches * pts, slots * BLK), lambda i, *_: (i, 0, 0)),
            scratch_shapes=[pltpu.VMEM((rows, pts, BLK), F32)],
        ),
        out_shape=jax.ShapeDtypeStruct((places, batches * pts, slots * BLK), BF16),
    )(rows_at, listed, gathered, points_t)


def line_field_kernel(tiles_at, tiles, basis, out, rows, *, slots):
    for place in range(out.shape[0]):
        first = (pl.program_id(0) * out.shape[0] + place) * slots
        for slot in range(slots):
            rows[place, slot * BLK : (slot + 1) * BLK, :] = tiles[tiles_at[first + slot]]
        out[place] = jnp.dot(basis[place], rows[place], preferred_element_type=F32)


def line_field(tiles_at, tiles, basis):
    places, points, functions = basis.shape
    count, _, width = tiles.shape
    step = min(STEP_PLACES, places)
    return call(
        functools.partial(line_field_kernel, slots=functions // BLK),
        "line_field",
        flops=2 * places * points * functions * width,
        grid_spec=pltpu.PrefetchScalarGridSpec(
            num_scalar_prefetch=1,
            grid=(places // step,),
            in_specs=[
                pl.BlockSpec((count, BLK, width), lambda i, *_: (0, 0, 0)),
                pl.BlockSpec((step, points, functions), lambda i, *_: (i, 0, 0)),
            ],
            out_specs=pl.BlockSpec((step, points, width), lambda i, *_: (i, 0, 0)),
            scratch_shapes=[pltpu.VMEM((step, functions, width), BF16)],
        ),
        out_shape=jax.ShapeDtypeStruct((places, points, width), F32),
    )(tiles_at, tiles, basis)


def one_hot(columns, rows):
    spot = lax.broadcasted_iota(jnp.int32, (rows, columns.shape[1]), 0)
    return jnp.where(spot == columns, 1.0, 0.0).astype(BF16)


def rejoin(picked):
    return picked[0:4] + picked[4:8] + picked[8:12]


def pair_kernel(target, source, window, local, points, out, spots):
    @pl.when(pl.program_id(1) == 0)
    def _():
        for axis in range(3):
            spots[axis] = jnp.broadcast_to(points[0, :, axis : axis + 1], spots.shape[1:])

    target_par = rejoin(
        jnp.dot(window[...], one_hot(target[0], window.shape[1]), preferred_element_type=F32)
    )
    source_par = rejoin(
        jnp.dot(local[...], one_hot(source[0], local.shape[1]), preferred_element_type=F32)
    )
    target_exp, source_exp = target_par[3:4], source_par[3:4]
    joined = target_exp + source_exp
    separation = jnp.zeros_like(joined)
    centres = []
    for axis in range(3):
        here, there = target_par[axis : axis + 1], source_par[axis : axis + 1]
        offset = here - there
        separation = separation + offset * offset
        centres.append((target_exp * here + source_exp * there) / joined)
    prefactor = 2.0 * math.pi / joined * jnp.exp(-target_exp * source_exp / joined * separation)
    lanes = spots.shape[2]
    for first in range(0, joined.shape[1], lanes):
        part = slice(first, first + lanes)
        spread = None
        for axis in range(3):
            delta = spots[axis] - centres[axis][:, part]
            spread = delta * delta if spread is None else spread + delta * delta
        argument = joined[:, part] * spread
        summed = jnp.zeros_like(argument)
        for quad_node in range(quad_nodes):
            node_spot = (quad_node + 0.5) / quad_nodes
            summed = summed + jnp.exp(-argument * (node_spot * node_spot))
        out[0, :, part] = prefactor[:, part] * (summed / quad_nodes)


def pair_values(target, source, window, local, points_t):
    batches, _, pairs = target.shape
    pts = points_t.shape[1]
    return call(
        pair_kernel,
        "pair_values",
        flops=batches * pairs * pts * 400,
        grid_spec=pltpu.PrefetchScalarGridSpec(
            num_scalar_prefetch=0,
            grid=(batches, pairs // CHUNK),
            in_specs=[
                pl.BlockSpec((1, 1, CHUNK), lambda b, n: (b, 0, n)),
                pl.BlockSpec((1, 1, CHUNK), lambda b, n: (b, 0, n)),
                pl.BlockSpec(window.shape, lambda b, n: (0, 0)),
                pl.BlockSpec(local.shape, lambda b, n: (0, 0)),
                pl.BlockSpec((1, pts, 3), lambda b, n: (b, 0, 0)),
            ],
            out_specs=pl.BlockSpec((1, pts, CHUNK), lambda b, n: (b, 0, n)),
            scratch_shapes=[pltpu.VMEM((3, pts, BLK), F32)],
        ),
        out_shape=jax.ShapeDtypeStruct((batches, pts, pairs), F32),
    )(target, source, window, local, points_t)


def potential_kernel(field, values, target, source, out, largest):
    columns, width = out.shape[0], out.shape[3]
    window_count = columns * width
    rounded = field[0].astype(BF16)
    potential = jnp.zeros((field.shape[1], window_count), F32)
    for first in range(0, values.shape[2], CHUNK):
        part = slice(first, first + CHUNK)
        picked = jnp.dot(rounded, one_hot(source[0, :, part], width), preferred_element_type=F32)
        product = (values[0, :, part] * picked).astype(BF16)
        potential += lax.dot_general(
            product,
            one_hot(target[0, :, part], window_count),
            (((1,), (1,)), ((), ())),
            preferred_element_type=F32,
        )
    for column in range(columns):
        out[column, 0] = potential[:, column * width : (column + 1) * width]
    largest[0] = jnp.broadcast_to(jnp.max(jnp.abs(potential), keepdims=True), largest.shape[1:])


def potential_parts(field, values, target, source, columns):
    batches, pts, width = field.shape
    pairs = values.shape[2]
    return call(
        potential_kernel,
        "potential_parts",
        flops=2 * batches * pts * pairs * columns * width,
        grid_spec=pltpu.PrefetchScalarGridSpec(
            num_scalar_prefetch=0,
            grid=(batches,),
            in_specs=[
                pl.BlockSpec((1, pts, width), lambda b: (b, 0, 0)),
                pl.BlockSpec((1, pts, pairs), lambda b: (b, 0, 0)),
                pl.BlockSpec((1, 1, pairs), lambda b: (b, 0, 0)),
                pl.BlockSpec((1, 1, pairs), lambda b: (b, 0, 0)),
            ],
            out_specs=[
                pl.BlockSpec((columns, 1, pts, width), lambda b: (0, b, 0, 0)),
                pl.BlockSpec((1, 8, BLK), lambda b: (b, 0, 0)),
            ],
        ),
        out_shape=[
            jax.ShapeDtypeStruct((columns, batches, pts, width), F32),
            jax.ShapeDtypeStruct((batches, 8, BLK), F32),
        ],
    )(field, values, target, source)


def owner_basis_kernel(pick, listed, points_at, params, gathered, *refs, batches):
    outs, spread_params = refs[:-1], refs[-1]
    together = batches // len(outs)

    @pl.when(pl.program_id(0) == 0)
    def _():
        for block in range(spread_params.shape[0]):
            for which in range(PARAMS):
                spread_params[block, which] = jnp.broadcast_to(
                    params[block * BLK : (block + 1) * BLK, which : which + 1], (BLK, BLK)
                )

    def one_owner(owner, carry):
        place = pl.program_id(0) * STEP_OWNERS + owner
        for slot in range(CAPB):
            block = pick[place * CAPB + slot]
            for batch in range(batches):
                out, lane = outs[batch // together], batch % together * BLK
                here = (owner, slice(slot * BLK, (slot + 1) * BLK), slice(lane, lane + BLK))
                keep = listed[(place * CAPB + slot) * batches + batch]

                @pl.when(keep > 0)
                def _(out=out, here=here):
                    squared = None
                    for axis in range(3):
                        row = points_at[place] + axis * batches + batch
                        delta = gathered[pl.ds(row, 1), :] - spread_params[block, axis]
                        squared = delta * delta if squared is None else squared + delta * delta
                    out[here] = jnp.exp(-spread_params[block, 3] * squared).astype(BF16)

                @pl.when(keep == 0)
                def _(out=out, here=here):
                    out[here] = jnp.zeros((BLK, BLK), BF16)

        return carry

    lax.fori_loop(0, STEP_OWNERS, one_owner, 0)


def basis_at_owner(pick, listed, points_at, params_t, gathered, batches, pts):
    owners = points_at.shape[0]
    held = params_t.shape[0] // BLK
    points = batches * pts // PARTS
    return call(
        functools.partial(owner_basis_kernel, batches=batches),
        "basis_at_owner",
        flops=owners * CAPB * BLK * batches * pts * 50,
        grid_spec=pltpu.PrefetchScalarGridSpec(
            num_scalar_prefetch=3,
            grid=(owners // STEP_OWNERS,),
            in_specs=[
                pl.BlockSpec(params_t.shape, lambda i, *_: (0, 0)),
                pl.BlockSpec(gathered.shape, lambda i, *_: (0, 0)),
            ],
            out_specs=[
                pl.BlockSpec((STEP_OWNERS, CAPB * BLK, points), lambda i, *_: (i, 0, 0))
            ]
            * PARTS,
            scratch_shapes=[pltpu.VMEM((held, PARAMS, BLK, BLK), F32)],
        ),
        out_shape=[jax.ShapeDtypeStruct((owners, CAPB * BLK, points), BF16)] * PARTS,
    )(pick, listed, points_at, params_t, gathered)


def add_rows(out, pick, place, rows):
    for slot in range(CAPB):
        block = pick[place * CAPB + slot]
        out[block] = out[block] + rows[slot * BLK : (slot + 1) * BLK]


def fock_kernel(pick, basis, weighted, before, out):
    @pl.when(pl.program_id(0) == 0)
    def _():
        out[...] = before[...]

    for owner in range(basis.shape[0]):
        place = pl.program_id(0) * basis.shape[0] + owner
        add_rows(out, pick, place, jnp.dot(basis[owner], weighted[owner], preferred_element_type=F32))


def fock_from_gather(pick, basis, weighted, before):
    owners, rows, points = basis.shape
    width = weighted.shape[2]
    step = min(STEP_GATHERED, owners)
    whole = pl.BlockSpec(before.shape, lambda i, *_: (0, 0, 0))
    return call(
        fock_kernel,
        "fock_from_gather",
        flops=2 * owners * rows * points * width,
        grid_spec=pltpu.PrefetchScalarGridSpec(
            num_scalar_prefetch=1,
            grid=(owners // step,),
            in_specs=[
                pl.BlockSpec((step, rows, points), lambda i, *_: (i, 0, 0)),
                pl.BlockSpec((step, points, width), lambda i, *_: (i, 0, 0)),
                whole,
            ],
            out_specs=whole,
        ),
        out_shape=jax.ShapeDtypeStruct(before.shape, F32),
        input_output_aliases={3: 0},
    )(pick, basis, weighted, before)


def fock_line_kernel(pick, lines, *refs, first, count, side, fresh):
    basis, weighted, out = refs[:count], refs[count : 2 * count], refs[-1]

    @pl.when(pl.program_id(0) == 0)
    def _():
        out[...] = jnp.zeros_like(out) if fresh else refs[2 * count][...]

    here = weighted[0].shape[0]
    for line in range(count):
        for owner in range(here):
            place = lines[first + line] * side + pl.program_id(0) * here + owner
            rows = jnp.dot(basis[line][owner], weighted[line][owner], preferred_element_type=F32)
            add_rows(out, pick, place, rows)


def fock_from_lines(pick, lines, first, basis, weighted, before, held):
    _, rows, points = basis.shape
    count = len(weighted)
    side, _, width = weighted[0].shape
    step = side // 2
    whole = pl.BlockSpec((held, BLK, width), lambda i, *_: (0, 0, 0))

    def line_spec(line):
        return pl.BlockSpec(
            (step, rows, points), lambda i, _, lines: (lines[first + line] * 2 + i, 0, 0)
        )

    return call(
        functools.partial(
            fock_line_kernel, first=first, count=count, side=side, fresh=before is None
        ),
        "fock_from_lines",
        flops=2 * count * side * rows * points * width,
        grid_spec=pltpu.PrefetchScalarGridSpec(
            num_scalar_prefetch=2,
            grid=(2,),
            in_specs=[line_spec(line) for line in range(count)]
            + [pl.BlockSpec((step, points, width), lambda i, *_: (i, 0, 0))] * count
            + ([] if before is None else [whole]),
            out_specs=whole,
        ),
        out_shape=jax.ShapeDtypeStruct((held, BLK, width), F32),
        input_output_aliases={} if before is None else {2 + 2 * count: 0},
    )(pick, lines, *[basis] * count, *weighted, *([] if before is None else [before]))


def to_everyone(value, axis):
    devices = lax.axis_size(axis)
    return lax.all_to_all(
        jnp.broadcast_to(value[None], (devices, *value.shape)), axis, 0, 0, tiled=True
    )


def in_parts(values):
    high = lax.reduce_precision(values, 8, 7)
    middle = lax.reduce_precision(values - high, 8, 7)
    low = values - high - middle
    parts = jnp.concatenate([high, middle, low, jnp.zeros_like(low)], axis=0)
    return parts.astype(BF16)


def sum_at_column(parts, largest):
    columns, batches, pts, width = parts.shape
    power = jnp.clip(13.0 - jnp.ceil(jnp.log2(largest)), -100.0, 100.0)
    scaled = (parts * jnp.exp2(power)[None, :, None, None]).astype(jnp.float16)
    tail = jnp.broadcast_to(
        power[None, :, None, None], (columns, batches, SCALE_ROWS, width)
    ).astype(jnp.float16)
    got = lax.all_to_all(
        jnp.concatenate([scaled, tail], axis=2), "col", split_axis=0, concat_axis=0, tiled=True
    )
    factor = jnp.exp2(-got[:, :, pts : pts + 1, 0:1].astype(F32))
    return jnp.sum(got[:, :, :pts].astype(F32) * factor, axis=0)


def slots_of(lists, base, held, batches):
    spot = lists - base
    owned = (spot >= 0) & (spot < held)
    lowest = jnp.min(jnp.where(owned, spot, held), axis=-1)
    highest = jnp.max(jnp.where(owned, spot, -1), axis=-1)
    ends = jnp.stack([lowest, highest], axis=-1)
    pick = jnp.where((highest >= 0)[..., None], ends, 0).astype(jnp.int32)
    hit = owned[..., None, :] & (spot[..., None, :] == ends[..., None])
    hit = hit & ((lowest != highest)[..., None] | (jnp.arange(CAPB) == 0))[..., None]
    listed = jnp.any(hit.reshape(*hit.shape[:-1], batches, -1), axis=-1)
    return pick, listed.astype(jnp.int32)


def on_device(
    density,
    row_centers,
    row_exps,
    win_centers,
    win_exps,
    points,
    weights,
    sig_blocks,
    pair_target,
    pair_source,
):
    lines, side = lax.axis_size("y"), lax.axis_size("z")
    owners = lines * side
    columns = lax.axis_size("col")
    line, place, column = lax.axis_index("y"), lax.axis_index("z"), lax.axis_index("col")
    held = row_exps.shape[0] // BLK
    width = density.shape[1]
    batches, _, pts = points.shape

    tiles = lax.all_gather(density, "z", axis=0, tiled=True).reshape(side * held, BLK, width)

    own_params = jnp.concatenate([row_centers, row_exps[None, :]], axis=0)
    own_blocks = own_params.reshape(PARAMS, held, BLK).transpose(1, 0, 2).reshape(columns, -1, BLK)
    block_rows = own_blocks.shape[1]
    own_points = points.transpose(1, 0, 2).reshape(3 * batches, pts)
    line_points = to_everyone(own_points, "y")
    point_rows = own_points.shape[0]
    shared = jnp.concatenate(
        [
            lax.dynamic_index_in_dim(own_blocks, column, 0, keepdims=False),
            lax.dynamic_index_in_dim(line_points, column, 0, keepdims=False),
        ],
        axis=0,
    )
    shared = to_everyone(shared, "z").reshape(-1, BLK)
    local_window = jnp.concatenate([win_centers, win_exps[None, :]], axis=0)
    spare = jnp.zeros_like(local_window)
    gathered = to_everyone(jnp.concatenate([shared, local_window, spare], axis=0), "col")
    rows_each = gathered.shape[1]
    whole_window = gathered[:, shared.shape[0] : shared.shape[0] + PARAMS]
    whole_window = whole_window.transpose(1, 0, 2).reshape(PARAMS, -1)
    gathered = gathered.reshape(-1, BLK)

    lists = sig_blocks.reshape(lines, side, -1)
    rows_of_place = block_rows + point_rows
    line_lists = lax.dynamic_index_in_dim(lists, place, 1, keepdims=True)
    base = (line * side + jnp.arange(side, dtype=jnp.int32)) * held
    line_pick, line_listed = slots_of(line_lists, base[None, :, None], held, batches)
    tiles_at = line_pick + (jnp.arange(side, dtype=jnp.int32) * held)[None, :, None]
    blocks_each = held // columns
    rows_at = (
        line_pick // blocks_each * rows_each
        + (jnp.arange(side, dtype=jnp.int32) * rows_of_place)[None, :, None]
        + line_pick % blocks_each * PARAMS
    )
    my_base = (line * side + place) * held
    pick, listed = slots_of(lists.reshape(owners, -1), my_base, held, batches)
    pick, listed = pick.reshape(-1), listed.reshape(-1)
    points_at = (
        jnp.arange(lines, dtype=jnp.int32)[:, None] * rows_each
        + jnp.arange(side, dtype=jnp.int32)[None, :] * rows_of_place
        + block_rows
    ).reshape(-1)

    points_t = points.transpose(0, 2, 1)
    target = pair_target[:, None, :]
    source = pair_source[:, None, :]
    basis = line_basis(
        rows_at.reshape(-1),
        line_listed.reshape(-1),
        gathered,
        line_points.transpose(0, 2, 1),
        batches,
    )
    share = line_field(tiles_at.reshape(-1), tiles, basis)
    share, local_window, whole_window, gathered = lax.optimization_barrier(
        (share, local_window, whole_window, gathered)
    )
    field = lax.psum_scatter(share.reshape(-1, width), "y", scatter_dimension=0, tiled=True)
    values = pair_values(target, source, in_parts(whole_window), in_parts(local_window), points_t)
    own_basis = basis_at_owner(pick, listed, points_at, own_params.T, gathered, batches, pts)
    values, own_basis = lax.optimization_barrier((values, own_basis))
    parts, largest = potential_parts(
        field.reshape(batches, pts, width), values, target, source, columns
    )
    potential = sum_at_column(parts, largest[:, 0, 0])
    weighted = (weights[:, :, None] * potential).astype(BF16).reshape(batches * pts, width)

    half = batches * pts // PARTS
    all_weighted = lax.all_gather(weighted[:half], GRID, axis=0, tiled=True)
    came = [to_everyone(weighted[half:], "z")]
    offsets = [0]
    for step in range(1, lines // 2 + 1):
        offsets += [lines - step, step]
    order = (line + jnp.array(offsets[:lines], jnp.int32)) & (lines - 1)
    ahead = [(i, (i + 1) % lines) for i in range(lines)]
    behind = [(i, (i - 1) % lines) for i in range(lines)]
    up = down = came[0]
    fock = None
    for step in range(1, lines // 2 + 1):
        up = lax.ppermute(up, "y", ahead)
        if step < lines - step:
            down = lax.ppermute(down, "y", behind)
        fock = fock_from_lines(pick, order, max(0, 2 * step - 3), own_basis[1], came, fock, held)
        if step < lines - step:
            up, down, fock = lax.optimization_barrier((up, down, fock))
            came = [up, down]
        else:
            fock = fock_from_lines(pick, order, 2 * step - 1, own_basis[1], [up], fock, held)
    fock = fock_from_gather(pick, own_basis[0], all_weighted.reshape(owners, half, width), fock)
    return fock.reshape(held * BLK, width)


def solution(mesh):
    columns = mesh.shape["col"]
    side = math.isqrt(mesh.shape["grid"])
    planes = Mesh(mesh.devices.reshape(-1, side, columns), (*GRID, "col"))
    return jax.shard_map(
        on_device,
        mesh=planes,
        in_specs=(
            P(GRID, "col"),
            P(None, GRID),
            P(GRID),
            P(None, "col"),
            P("col"),
            P(GRID, None, None),
            P(GRID, None),
            P(),
            P(GRID, "col"),
            P(GRID, "col"),
        ),
        out_specs=P(GRID, "col"),
        check_vma=False,
    )
```

```python
import functools
import math

import jax
import jax.numpy as jnp
from jax import lax
from jax.experimental import pallas as pl
from jax.experimental.pallas import tpu as pltpu
from jax.sharding import Mesh
from jax.sharding import PartitionSpec as P

BLK = 128
CAPB = 2
PARAMS = 4
CHUNK = 512
STEP_OWNERS = 4
SCALE_ROWS = 8
STEP_GATHERED = 16
STEP_PLACES = 2
GRID = ("y", "z")
quad_nodes = 8
F32 = jnp.float32
BF16 = jnp.bfloat16


def call(kernel, name, flops=0, **kwargs):
    return pl.pallas_call(
        kernel,
        name=name,
        compiler_params=pltpu.CompilerParams(
            dimension_semantics=("arbitrary",) * len(kwargs["grid_spec"].grid),
        ),
        cost_estimate=pl.CostEstimate(flops=flops, transcendentals=0, bytes_accessed=0),
        **kwargs,
    )


def line_basis_kernel(rows_at, listed, gathered, points, out, spots, *, batches, slots):
    place = pl.program_id(0)
    for row in range(3 * batches):
        spots[row] = jnp.broadcast_to(points[0, :, row : row + 1], spots.shape[1:])

    def one_slot(slot, carry):
        row = rows_at[place * slots + slot]
        lanes = pl.ds(pl.multiple_of(slot * BLK, BLK), BLK)
        for batch in range(batches):
            keep = listed[(place * slots + slot) * batches + batch]
            here = (0, slice(batch * BLK, (batch + 1) * BLK), lanes)

            @pl.when(keep > 0)
            def _():
                squared = None
                for axis in range(3):
                    delta = spots[axis * batches + batch] - gathered[pl.ds(row + axis, 1), :]
                    squared = delta * delta if squared is None else squared + delta * delta
                out[here] = jnp.exp(-gathered[pl.ds(row + 3, 1), :] * squared).astype(BF16)

            @pl.when(keep == 0)
            def _():
                out[here] = jnp.zeros((BLK, BLK), BF16)

        return carry

    lax.fori_loop(0, slots, one_slot, 0)


def line_basis(rows_at, listed, gathered, points_t, batches):
    places, pts, rows = points_t.shape
    slots = rows_at.shape[0] // places
    return call(
        functools.partial(line_basis_kernel, batches=batches, slots=slots),
        "line_basis",
        flops=places * batches * pts * slots * BLK * 50,
        grid_spec=pltpu.PrefetchScalarGridSpec(
            num_scalar_prefetch=2,
            grid=(places,),
            in_specs=[
                pl.BlockSpec(gathered.shape, lambda i, *_: (0, 0)),
                pl.BlockSpec((1, pts, rows), lambda i, *_: (i, 0, 0)),
            ],
            out_specs=pl.BlockSpec((1, batches * pts, slots * BLK), lambda i, *_: (i, 0, 0)),
            scratch_shapes=[pltpu.VMEM((rows, pts, BLK), F32)],
        ),
        out_shape=jax.ShapeDtypeStruct((places, batches * pts, slots * BLK), BF16),
    )(rows_at, listed, gathered, points_t)


def line_field_kernel(tiles_at, tiles, basis, out, rows, *, slots):
    for place in range(out.shape[0]):
        first = (pl.program_id(0) * out.shape[0] + place) * slots
        for slot in range(slots):
            rows[place, slot * BLK : (slot + 1) * BLK, :] = tiles[tiles_at[first + slot]]
        out[place] = jnp.dot(basis[place], rows[place], preferred_element_type=F32)


def line_field(tiles_at, tiles, basis):
    places, points, functions = basis.shape
    count, _, width = tiles.shape
    step = min(STEP_PLACES, places)
    return call(
        functools.partial(line_field_kernel, slots=functions // BLK),
        "line_field",
        flops=2 * places * points * functions * width,
        grid_spec=pltpu.PrefetchScalarGridSpec(
            num_scalar_prefetch=1,
            grid=(places // step,),
            in_specs=[
                pl.BlockSpec((count, BLK, width), lambda i, *_: (0, 0, 0)),
                pl.BlockSpec((step, points, functions), lambda i, *_: (i, 0, 0)),
            ],
            out_specs=pl.BlockSpec((step, points, width), lambda i, *_: (i, 0, 0)),
            scratch_shapes=[pltpu.VMEM((step, functions, width), BF16)],
        ),
        out_shape=jax.ShapeDtypeStruct((places, points, width), F32),
    )(tiles_at, tiles, basis)


def one_hot(columns, rows):
    spot = lax.broadcasted_iota(jnp.int32, (rows, columns.shape[1]), 0)
    return jnp.where(spot == columns, 1.0, 0.0).astype(BF16)


def rejoin(picked):
    return picked[0:4] + picked[4:8] + picked[8:12]


def pair_kernel(target, source, window, local, points, out, spots):
    @pl.when(pl.program_id(1) == 0)
    def _():
        for axis in range(3):
            spots[axis] = jnp.broadcast_to(points[0, :, axis : axis + 1], spots.shape[1:])

    target_par = rejoin(
        jnp.dot(window[...], one_hot(target[0], window.shape[1]), preferred_element_type=F32)
    )
    source_par = rejoin(
        jnp.dot(local[...], one_hot(source[0], local.shape[1]), preferred_element_type=F32)
    )
    target_exp, source_exp = target_par[3:4], source_par[3:4]
    joined = target_exp + source_exp
    separation = jnp.zeros_like(joined)
    centres = []
    for axis in range(3):
        here, there = target_par[axis : axis + 1], source_par[axis : axis + 1]
        offset = here - there
        separation = separation + offset * offset
        centres.append((target_exp * here + source_exp * there) / joined)
    prefactor = 2.0 * math.pi / joined * jnp.exp(-target_exp * source_exp / joined * separation)
    lanes = spots.shape[2]
    for first in range(0, joined.shape[1], lanes):
        part = slice(first, first + lanes)
        spread = None
        for axis in range(3):
            delta = spots[axis] - centres[axis][:, part]
            spread = delta * delta if spread is None else spread + delta * delta
        argument = joined[:, part] * spread
        summed = jnp.zeros_like(argument)
        for quad_node in range(quad_nodes):
            node_spot = (quad_node + 0.5) / quad_nodes
            summed = summed + jnp.exp(-argument * (node_spot * node_spot))
        out[0, :, part] = prefactor[:, part] * (summed / quad_nodes)


def pair_values(target, source, window, local, points_t):
    batches, _, pairs = target.shape
    pts = points_t.shape[1]
    return call(
        pair_kernel,
        "pair_values",
        flops=batches * pairs * pts * 400,
        grid_spec=pltpu.PrefetchScalarGridSpec(
            num_scalar_prefetch=0,
            grid=(batches, pairs // CHUNK),
            in_specs=[
                pl.BlockSpec((1, 1, CHUNK), lambda b, n: (b, 0, n)),
                pl.BlockSpec((1, 1, CHUNK), lambda b, n: (b, 0, n)),
                pl.BlockSpec(window.shape, lambda b, n: (0, 0)),
                pl.BlockSpec(local.shape, lambda b, n: (0, 0)),
                pl.BlockSpec((1, pts, 3), lambda b, n: (b, 0, 0)),
            ],
            out_specs=pl.BlockSpec((1, pts, CHUNK), lambda b, n: (b, 0, n)),
            scratch_shapes=[pltpu.VMEM((3, pts, BLK), F32)],
        ),
        out_shape=jax.ShapeDtypeStruct((batches, pts, pairs), F32),
    )(target, source, window, local, points_t)


def potential_kernel(field, values, target, source, out):
    columns, width = out.shape[0], out.shape[3]
    window_count = columns * width
    rounded = field[0].astype(BF16)
    potential = jnp.zeros((field.shape[1], window_count), F32)
    for first in range(0, values.shape[2], CHUNK):
        part = slice(first, first + CHUNK)
        picked = jnp.dot(rounded, one_hot(source[0, :, part], width), preferred_element_type=F32)
        product = (values[0, :, part] * picked).astype(BF16)
        potential += lax.dot_general(
            product,
            one_hot(target[0, :, part], window_count),
            (((1,), (1,)), ((), ())),
            preferred_element_type=F32,
        )
    largest = jnp.max(jnp.abs(potential), keepdims=True)
    power = jnp.clip(13.0 - jnp.ceil(jnp.log2(largest)), -100.0, 100.0)
    scaled = potential * jnp.exp2(power)
    pts = potential.shape[0]
    for column in range(columns):
        out[column, 0, :pts] = scaled[:, column * width : (column + 1) * width]
        out[column, 0, pts:] = jnp.broadcast_to(power, (SCALE_ROWS, width))


def potential_parts(field, values, target, source, columns):
    batches, pts, width = field.shape
    pairs = values.shape[2]
    return call(
        potential_kernel,
        "potential_parts",
        flops=2 * batches * pts * pairs * columns * width,
        grid_spec=pltpu.PrefetchScalarGridSpec(
            num_scalar_prefetch=0,
            grid=(batches,),
            in_specs=[
                pl.BlockSpec((1, pts, width), lambda b: (b, 0, 0)),
                pl.BlockSpec((1, pts, pairs), lambda b: (b, 0, 0)),
                pl.BlockSpec((1, 1, pairs), lambda b: (b, 0, 0)),
                pl.BlockSpec((1, 1, pairs), lambda b: (b, 0, 0)),
            ],
            out_specs=pl.BlockSpec((columns, 1, pts + SCALE_ROWS, width), lambda b: (0, b, 0, 0)),
        ),
        out_shape=jax.ShapeDtypeStruct((columns, batches, pts + SCALE_ROWS, width), F32),
    )(field, values, target, source)


def owner_basis_kernel(pick, listed, points_at, params, gathered, out, spread_params, *, batches):
    @pl.when(pl.program_id(0) == 0)
    def _():
        for block in range(spread_params.shape[0]):
            for which in range(PARAMS):
                spread_params[block, which] = jnp.broadcast_to(
                    params[block * BLK : (block + 1) * BLK, which : which + 1], (BLK, BLK)
                )

    def one_owner(owner, carry):
        place = pl.program_id(0) * STEP_OWNERS + owner
        for slot in range(CAPB):
            block = pick[place * CAPB + slot]
            for batch in range(batches):
                here = (owner, slice(slot * BLK, (slot + 1) * BLK), slice(batch * BLK, (batch + 1) * BLK))
                keep = listed[(place * CAPB + slot) * batches + batch]

                @pl.when(keep > 0)
                def _():
                    squared = None
                    for axis in range(3):
                        row = points_at[place] + axis * batches + batch
                        delta = gathered[pl.ds(row, 1), :] - spread_params[block, axis]
                        squared = delta * delta if squared is None else squared + delta * delta
                    out[here] = jnp.exp(-spread_params[block, 3] * squared).astype(BF16)

                @pl.when(keep == 0)
                def _():
                    out[here] = jnp.zeros((BLK, BLK), BF16)

        return carry

    lax.fori_loop(0, STEP_OWNERS, one_owner, 0)


def basis_at_owner(pick, listed, points_at, params_t, gathered, batches, pts):
    owners = points_at.shape[0]
    held = params_t.shape[0] // BLK
    return call(
        functools.partial(owner_basis_kernel, batches=batches),
        "basis_at_owner",
        flops=owners * CAPB * BLK * batches * pts * 50,
        grid_spec=pltpu.PrefetchScalarGridSpec(
            num_scalar_prefetch=3,
            grid=(owners // STEP_OWNERS,),
            in_specs=[
                pl.BlockSpec(params_t.shape, lambda i, *_: (0, 0)),
                pl.BlockSpec(gathered.shape, lambda i, *_: (0, 0)),
            ],
            out_specs=pl.BlockSpec((STEP_OWNERS, CAPB * BLK, batches * pts), lambda i, *_: (i, 0, 0)),
            scratch_shapes=[pltpu.VMEM((held, PARAMS, BLK, BLK), F32)],
        ),
        out_shape=jax.ShapeDtypeStruct((owners, CAPB * BLK, batches * pts), BF16),
    )(pick, listed, points_at, params_t, gathered)


def add_rows(out, pick, place, rows):
    for slot in range(CAPB):
        block = pick[place * CAPB + slot]
        out[block] = out[block] + rows[slot * BLK : (slot + 1) * BLK]


def fock_kernel(pick, basis, weighted, out):
    @pl.when(pl.program_id(0) == 0)
    def _():
        out[...] = jnp.zeros_like(out)

    for owner in range(basis.shape[0]):
        place = pl.program_id(0) * basis.shape[0] + owner
        add_rows(out, pick, place, jnp.dot(basis[owner], weighted[owner], preferred_element_type=F32))


def fock_at_owner(pick, basis, weighted, held):
    owners, rows, points = basis.shape
    width = weighted.shape[2]
    step = min(STEP_GATHERED, owners)
    return call(
        fock_kernel,
        "fock_at_owner",
        flops=2 * owners * rows * points * width,
        grid_spec=pltpu.PrefetchScalarGridSpec(
            num_scalar_prefetch=1,
            grid=(owners // step,),
            in_specs=[
                pl.BlockSpec((step, rows, points), lambda i, *_: (i, 0, 0)),
                pl.BlockSpec((step, points, width), lambda i, *_: (i, 0, 0)),
            ],
            out_specs=pl.BlockSpec((held, BLK, width), lambda i, *_: (0, 0, 0)),
        ),
        out_shape=jax.ShapeDtypeStruct((held, BLK, width), F32),
    )(pick, basis, weighted)


def to_everyone(value, axis):
    devices = lax.axis_size(axis)
    return lax.all_to_all(
        jnp.broadcast_to(value[None], (devices, *value.shape)), axis, 0, 0, tiled=True
    )


def in_parts(values):
    high = lax.reduce_precision(values, 8, 7)
    middle = lax.reduce_precision(values - high, 8, 7)
    low = values - high - middle
    parts = jnp.concatenate([high, middle, low, jnp.zeros_like(low)], axis=0)
    return parts.astype(BF16)


def sum_at_column(parts):
    pts = parts.shape[2] - SCALE_ROWS
    got = lax.all_to_all(
        parts.astype(jnp.float16), "col", split_axis=0, concat_axis=0, tiled=True
    )
    factor = jnp.exp2(-got[:, :, pts : pts + 1, 0:1].astype(F32))
    return jnp.sum(got[:, :, :pts].astype(F32) * factor, axis=0)


def slots_of(lists, base, held, batches):
    spot = lists - base
    owned = (spot >= 0) & (spot < held)
    lowest = jnp.min(jnp.where(owned, spot, held), axis=-1)
    highest = jnp.max(jnp.where(owned, spot, -1), axis=-1)
    ends = jnp.stack([lowest, highest], axis=-1)
    pick = jnp.where((highest >= 0)[..., None], ends, 0).astype(jnp.int32)
    hit = owned[..., None, :] & (spot[..., None, :] == ends[..., None])
    hit = hit & ((lowest != highest)[..., None] | (jnp.arange(CAPB) == 0))[..., None]
    listed = jnp.any(hit.reshape(*hit.shape[:-1], batches, -1), axis=-1)
    return pick, listed.astype(jnp.int32)


def on_device(
    density,
    row_centers,
    row_exps,
    win_centers,
    win_exps,
    points,
    weights,
    sig_blocks,
    pair_target,
    pair_source,
):
    lines, side = lax.axis_size("y"), lax.axis_size("z")
    owners = lines * side
    columns = lax.axis_size("col")
    line, place, column = lax.axis_index("y"), lax.axis_index("z"), lax.axis_index("col")
    held = row_exps.shape[0] // BLK
    width = density.shape[1]
    batches, _, pts = points.shape

    tiles = lax.all_gather(density, "z", axis=0, tiled=True).reshape(side * held, BLK, width)

    own_params = jnp.concatenate([row_centers, row_exps[None, :]], axis=0)
    own_blocks = own_params.reshape(PARAMS, held, BLK).transpose(1, 0, 2).reshape(columns, -1, BLK)
    block_rows = own_blocks.shape[1]
    own_points = points.transpose(1, 0, 2).reshape(3 * batches, pts)
    line_points = to_everyone(own_points, "y")
    point_rows = own_points.shape[0]
    shared = jnp.concatenate(
        [
            lax.dynamic_index_in_dim(own_blocks, column, 0, keepdims=False),
            lax.dynamic_index_in_dim(line_points, column, 0, keepdims=False),
        ],
        axis=0,
    )
    shared = to_everyone(shared, "z").reshape(-1, BLK)
    local_window = jnp.concatenate([win_centers, win_exps[None, :]], axis=0)
    spare = jnp.zeros_like(local_window)
    gathered = to_everyone(jnp.concatenate([shared, local_window, spare], axis=0), "col")
    rows_each = gathered.shape[1]
    whole_window = gathered[:, shared.shape[0] : shared.shape[0] + PARAMS]
    whole_window = whole_window.transpose(1, 0, 2).reshape(PARAMS, -1)
    gathered = gathered.reshape(-1, BLK)

    lists = sig_blocks.reshape(lines, side, -1)
    rows_of_place = block_rows + point_rows
    line_lists = lax.dynamic_index_in_dim(lists, place, 1, keepdims=True)
    base = (line * side + jnp.arange(side, dtype=jnp.int32)) * held
    line_pick, line_listed = slots_of(line_lists, base[None, :, None], held, batches)
    tiles_at = line_pick + (jnp.arange(side, dtype=jnp.int32) * held)[None, :, None]
    blocks_each = held // columns
    rows_at = (
        line_pick // blocks_each * rows_each
        + (jnp.arange(side, dtype=jnp.int32) * rows_of_place)[None, :, None]
        + line_pick % blocks_each * PARAMS
    )
    my_base = (line * side + place) * held
    pick, listed = slots_of(lists.reshape(owners, -1), my_base, held, batches)
    pick, listed = pick.reshape(-1), listed.reshape(-1)
    points_at = (
        jnp.arange(lines, dtype=jnp.int32)[:, None] * rows_each
        + jnp.arange(side, dtype=jnp.int32)[None, :] * rows_of_place
        + block_rows
    ).reshape(-1)

    points_t = points.transpose(0, 2, 1)
    target = pair_target[:, None, :]
    source = pair_source[:, None, :]
    basis = line_basis(
        rows_at.reshape(-1),
        line_listed.reshape(-1),
        gathered,
        line_points.transpose(0, 2, 1),
        batches,
    )
    share = line_field(tiles_at.reshape(-1), tiles, basis)
    share, local_window, whole_window = lax.optimization_barrier(
        (share, local_window, whole_window)
    )
    field = lax.psum_scatter(share.reshape(-1, width), "y", scatter_dimension=0, tiled=True)
    values = pair_values(target, source, in_parts(whole_window), in_parts(local_window), points_t)
    parts = potential_parts(
        field.reshape(batches, pts, width), values, target, source, columns
    )
    potential = sum_at_column(parts)
    weighted = (weights[:, :, None] * potential).astype(BF16).reshape(batches * pts, width)

    all_weighted = lax.all_gather(weighted, GRID, axis=0, tiled=True)
    gathered, weighted = lax.optimization_barrier((gathered, weighted))
    own_basis = basis_at_owner(pick, listed, points_at, own_params.T, gathered, batches, pts)
    fock = fock_at_owner(
        pick, own_basis, all_weighted.reshape(owners, batches * pts, width), held
    )
    return fock.reshape(held * BLK, width)


def solution(mesh):
    columns = mesh.shape["col"]
    side = math.isqrt(mesh.shape["grid"])
    planes = Mesh(mesh.devices.reshape(-1, side, columns), (*GRID, "col"))
    return jax.shard_map(
        on_device,
        mesh=planes,
        in_specs=(
            P(GRID, "col"),
            P(None, GRID),
            P(GRID),
            P(None, "col"),
            P("col"),
            P(GRID, None, None),
            P(GRID, None),
            P(),
            P(GRID, "col"),
            P(GRID, "col"),
        ),
        out_specs=P(GRID, "col"),
        check_vma=False,
    )
```
